32 devices in a mesh: ta: 2 (over x), gx: 16 (over z, y, core).
Axes of the slice: x: 2, y: 2, z: 4, core: 2. Of those that a mesh axis runs over, the one named last changes fastest.
Arguments:
- voltages: bfloat16 [2, 128, 2, 256, 512], P('ta', 'gx'), may hold values from -6 to 6
- weights: bfloat16 [2, 256, 2, 512, 64], P(None, 'gx'), may hold values from -0.125 to 0.125
Outputs:
- spectra: float32 [256, 2, 512, 64], P(None, None, 'gx', 'ta')
The draws below stay inside these ranges and needn't reach their ends.
All inputs are finite; a program needn't handle non-finite values.
Results may differ from the reference program's by a relative error of at most 0.0003.
Values may be sent and summed in bfloat16 or wider, within the bound.
A program may use at most 64 MiB of HBM per device.

```python
import jax
import jax.numpy as jnp
from jax import lax

ANTENNA_COUNT = 64
BEAM_TOTAL = 512
CHANNEL_COUNT = 512
HALF_SAMPLES = 512


def block_levels(own_key, shape, cuts, low, largest):
    factor_of = 1.0
    for position, blocks in cuts:
        draws = jax.random.uniform(jax.random.fold_in(jax.random.fold_in(own_key, 6), position), (blocks,), jnp.float32, low / len(cuts), largest / len(cuts))
        factor_of = factor_of * jnp.repeat(jnp.exp(draws), shape[position] // blocks).reshape((-1,) + (1,) * (len(shape) - 1 - position))
    return factor_of


def normal_values(rng, dims, scale, most, pieces=(), dtype=jnp.bfloat16):
    array = scale * jax.random.normal(rng, dims, jnp.float32)
    if pieces:
        array = array * block_levels(rng, dims, pieces, -0.22, 0.18)
    return jnp.clip(array, -most, most).astype(dtype)


def setup_inputs(seed: int = 0) -> dict:
    streams_of = jax.random.split(jax.random.key(seed), 3)
    voltages = normal_values(streams_of[0], (2, 2 * ANTENNA_COUNT, 2, CHANNEL_COUNT // 2, HALF_SAMPLES), 1.0, 6.0, ((0, 2), (1, 16)))
    weights = normal_values(streams_of[1], (2, CHANNEL_COUNT // 2, 2, BEAM_TOTAL, ANTENNA_COUNT), (32 * ANTENNA_COUNT) ** -0.5, 0.125, ((1, 16),))
    return dict(voltages=voltages, weights=weights)


def beam_power(voltage, weight_block):
    antennas = weight_block.shape[3]
    beam_count = weight_block.shape[2]
    powers = []
    for side_index in range(2):
        real_w = weight_block[side_index, 0]
        imag_w = weight_block[side_index, 1]
        upper_rows = jnp.stack([real_w, -imag_w], axis=-1).reshape(beam_count, 2 * antennas)
        bottom_half_rows = jnp.stack([imag_w, real_w], axis=-1).reshape(beam_count, 2 * antennas)
        matrix = jnp.concatenate([upper_rows, bottom_half_rows], 0)
        signal = voltage[side_index * antennas:(side_index + 1) * antennas].reshape(2 * antennas, -1)
        beam_voltage_field = jnp.dot(matrix, signal, preferred_element_type=jnp.float32)
        power = beam_voltage_field[:beam_count] * beam_voltage_field[:beam_count] + beam_voltage_field[beam_count:] * beam_voltage_field[beam_count:]
        powers.append(power.reshape(beam_count, -1, 8).sum(-1))
    return jnp.stack(powers, 0)


def reference(voltages, weights):
    moved = jnp.moveaxis(voltages, 3, 0)
    weight_moved = jnp.moveaxis(weights, 1, 0)

    def one_channel(paired):
        voltage, weight_block = paired
        return beam_power(voltage[0], weight_block) + beam_power(voltage[1], weight_block)

    return lax.map(one_channel, (moved, weight_moved))
```

```python
import functools

import jax
import jax.numpy as jnp
import numpy as np
from jax import lax
from jax.experimental import pallas as pl
from jax.experimental.pallas import tpu as pltpu
from jax.sharding import PartitionSpec as P

BF16 = np.dtype(jnp.bfloat16)
MESH = pl.DeviceIdType.MESH
CHUNKS = 4
PIECES = 4
LEAD = 2
TOP = 2.0**15.75
FLOOR = 2.0**-90


def beam_power(voltage, weight_block):
    antennas = weight_block.shape[3]
    beam_count = weight_block.shape[2]
    powers = []
    for side_index in range(2):
        real_w = weight_block[side_index, 0]
        imag_w = weight_block[side_index, 1]
        upper_rows = jnp.stack([real_w, -imag_w], axis=-1).reshape(beam_count, 2 * antennas)
        bottom_half_rows = jnp.stack([imag_w, real_w], axis=-1).reshape(beam_count, 2 * antennas)
        matrix = jnp.concatenate([upper_rows, bottom_half_rows], 0)
        signal = voltage[side_index * antennas : (side_index + 1) * antennas].reshape(
            2 * antennas, -1
        )
        beam_voltage_field = jnp.dot(matrix, signal, preferred_element_type=jnp.float32)
        power = (
            beam_voltage_field[:beam_count] * beam_voltage_field[:beam_count]
            + beam_voltage_field[beam_count:] * beam_voltage_field[beam_count:]
        )
        powers.append(power.reshape(beam_count, -1, 8).sum(-1))
    return jnp.stack(powers, 0)


def channel_powers(turned, weights):

    def one_channel(column):
        voltage = lax.dynamic_index_in_dim(turned, column, 2, keepdims=False)
        weight_block = lax.dynamic_index_in_dim(weights, column, 1, keepdims=False)
        return beam_power(voltage, weight_block)

    return lax.map(one_channel, jnp.arange(turned.shape[2], dtype=jnp.int32))


def plain_on_device(voltages, weights):
    turned = lax.all_to_all(voltages, "gx", split_axis=3, concat_axis=1, tiled=True)
    partial_power_value = channel_powers(turned[0], weights)
    relaid = lax.all_to_all(partial_power_value, "gx", split_axis=2, concat_axis=0, tiled=True)
    return lax.psum_scatter(relaid, "ta", scatter_dimension=3, tiled=True)


def kernel(
    nx, ng, v_ref, w_hbm, turn_ref, mix_ref, gather_ref, out_ref, peak_ref,
    sbuf, vrecv, w_ref, work, pbuf, peaks,
    w_sem, wsend, wz, relay_sem, wx, vsend, vget, psend, pget, msend, mget,
):
    x = lax.axis_index("ta")
    g = lax.axis_index("gx")
    me = x * ng + g
    n = nx * ng
    rows = v_ref.shape[0] * v_ref.shape[1]
    chans = v_ref.shape[2] // ng
    half = v_ref.shape[3] // nx
    per = chans // CHUNKS
    group = ng // 2
    antennas2 = group * rows
    beams = w_ref.shape[4]
    side = g // group
    u = lax.rem(g, group)
    partner = lax.rem(g + group, ng)
    steps = 2 * CHUNKS
    dests = nx * group
    mine = x * group + u
    piece = chans // nx // PIECES

    w_copy = pltpu.make_async_copy(w_hbm.at[side], w_ref.at[0], w_sem)
    w_copy.start()

    barrier = pltpu.get_barrier_semaphore()

    def greet(i, _):
        d = lax.rem(me + i, n)
        pl.semaphore_signal(
            barrier, inc=1, device_id=(d // ng, lax.rem(d, ng)), device_id_type=MESH
        )
        return 0

    lax.fori_loop(1, n, greet, 0)

    def turn_side(which):
        base = lax.rem(which + side, 2) * CHUNKS

        def turn(i, _):
            start = pl.multiple_of((which * group + i) * chans, chans)
            block = v_ref[:, :, pl.ds(start, chans), :].reshape(rows * chans, nx * half)
            turned = jnp.dot(turn_ref[...], block, preferred_element_type=jnp.float32)
            turned = turned.astype(jnp.bfloat16).reshape(CHUNKS, per, rows, nx * half)
            for k in range(nx):
                sbuf[pl.ds(base, CHUNKS), k * group + i] = turned[
                    :, :, :, k * half : (k + 1) * half
                ]
            return 0

        lax.fori_loop(0, group, turn, 0)

    def send_voltages(k):
        pltpu.make_async_copy(sbuf.at[k, mine], vrecv.at[k, mine], vget.at[k]).start()

        def send(i, _):
            d = lax.rem(mine + i, dests)
            pltpu.make_async_remote_copy(
                src_ref=sbuf.at[k, d],
                dst_ref=vrecv.at[k, mine],
                send_sem=vsend.at[k],
                recv_sem=vget.at[k],
                device_id=(d // group, side * group + lax.rem(d, group)),
                device_id_type=MESH,
            ).start()
            return 0

        lax.fori_loop(1, dests, send, 0)

    def send_weights(i):
        span = pl.ds((x * PIECES + i) * piece, piece)
        pltpu.make_async_remote_copy(
            src_ref=w_hbm.at[1 - side, span],
            dst_ref=w_ref.at[1, span],
            send_sem=wsend,
            recv_sem=wz.at[i],
            device_id=(x, partner),
            device_id_type=MESH,
        ).start()

    def relay_weights(i):
        block = w_ref.at[1, pl.ds((x * PIECES + i) * piece, piece)]
        pltpu.make_async_copy(block, block, wz.at[i]).wait()
        pltpu.make_async_remote_copy(
            src_ref=block,
            dst_ref=block,
            send_sem=relay_sem,
            recv_sem=wx,
            device_id=(1 - x, g),
            device_id_type=MESH,
        ).start()

    turn_side(side)
    pl.semaphore_wait(barrier, n - 1)
    for k in range(LEAD):
        send_voltages(k)
        send_weights(k)
    turn_side(1 - side)
    w_copy.wait()

    def step(k, _):
        pltpu.make_async_copy(vrecv.at[k], vrecv.at[k], vget.at[k]).wait()

        @pl.when(k + LEAD < steps)
        def _():
            send_voltages(k + LEAD)

        @pl.when(k + LEAD < PIECES)
        def _():
            send_weights(k + LEAD)

        @pl.when((k >= 1) & (k <= PIECES))
        def _():
            relay_weights(k - 1)

        @pl.when(k == CHUNKS)
        def _():
            other = w_ref.at[1, pl.ds((1 - x) * PIECES * piece, PIECES * piece)]
            pltpu.make_async_copy(other, other, wx).wait()

        which = k // CHUNKS
        part_of = lax.rem(k, CHUNKS)

        def channel(c, peak):
            w = w_ref[which, part_of * per + c].reshape(antennas2, beams).T
            power = None
            for h in range(nx):
                v = vrecv[k, h * group : (h + 1) * group, c].reshape(antennas2, half)
                mixed = jnp.dot(mix_ref[...], v, preferred_element_type=jnp.float32)
                mixed = mixed.astype(jnp.bfloat16)
                re = jnp.dot(w, mixed[:antennas2], preferred_element_type=jnp.float32)
                im = jnp.dot(w, mixed[antennas2:], preferred_element_type=jnp.float32)
                part = re * re + im * im
                power = part if power is None else power + part
            own = beams // ng
            packs = own // 8
            power = power.reshape(ng, packs, 8, half)
            total = None
            for m in range(packs):
                p = power[:, m].reshape(ng * 8, half)
                high = p.astype(jnp.bfloat16)
                low = (p - high.astype(jnp.float32)).astype(jnp.bfloat16)
                t = jnp.dot(high, gather_ref[m], preferred_element_type=jnp.float32)
                t += jnp.dot(low, gather_ref[m], preferred_element_type=jnp.float32)
                total = t if total is None else total + t
            total = total.reshape(ng, 8, 128)
            work[:, pl.ds(c, 1)] = total[:, None]
            return jnp.maximum(peak, jnp.max(total, axis=0))

        peak = lax.fori_loop(0, per, channel, jnp.zeros((8, 128), jnp.float32))
        peak = jnp.maximum(jnp.max(peak, keepdims=True), FLOOR)
        code = work[...].reshape(ng, per * 8, 128) * (TOP / peak)[None]
        code = code * code
        code = code * code
        pbuf[k] = (code * code).astype(jnp.bfloat16)
        row = lax.broadcasted_iota(jnp.int32, peaks.shape, 0)
        lane = lax.broadcasted_iota(jnp.int32, peaks.shape, 1)
        own_row = lax.rem(side + which, 2)
        first = u * chans + part_of * per
        held = (row == own_row) & (lane >= first) & (lane < first + per)
        peaks[...] = jnp.where(held, peak, peaks[...])

        target = out_ref.at[side, lax.rem(g + which * group, ng), part_of]
        pltpu.make_async_copy(pbuf.at[k, g], target, pget).start()

        def send(i, _):
            d = lax.rem(g + i, ng)
            pltpu.make_async_remote_copy(
                src_ref=pbuf.at[k, d],
                dst_ref=target,
                send_sem=psend,
                recv_sem=pget,
                device_id=(x, d),
                device_id_type=MESH,
            ).start()
            return 0

        lax.fori_loop(1, ng, send, 0)
        return 0

    peaks[...] = jnp.zeros_like(peaks)
    lax.fori_loop(0, steps, step, 0)

    pltpu.make_async_copy(peaks, peak_ref.at[side, u], mget).start()

    def send_peaks(i, _):
        pltpu.make_async_remote_copy(
            src_ref=peaks,
            dst_ref=peak_ref.at[side, u],
            send_sem=msend,
            recv_sem=mget,
            device_id=(x, lax.rem(g + i, ng)),
            device_id_type=MESH,
        ).start()
        return 0

    lax.fori_loop(1, ng, send_peaks, 0)

    pltpu.make_async_copy(peak_ref, peak_ref, mget).wait()
    pltpu.make_async_copy(out_ref, out_ref, pget).wait()
    for k in range(steps):
        sent = sbuf.at[k, pl.ds(0, dests - 1)]
        pltpu.make_async_copy(sent, sent, vsend.at[k]).wait()
    sent = pbuf.at[:, pl.ds(0, ng - 1)]
    pltpu.make_async_copy(sent, sent, psend).wait()
    sent = peak_ref.at[:, pl.ds(0, group - 1)]
    pltpu.make_async_copy(sent, sent, msend).wait()
    sent = peak_ref.at[0, pl.ds(0, 1)]
    pltpu.make_async_copy(sent, sent, msend).wait()
    sent = w_ref.at[1, pl.ds(0, PIECES * piece)]
    pltpu.make_async_copy(sent, sent, wsend).wait()
    pltpu.make_async_copy(sent, sent, relay_sem).wait()


def spread_kernel(in_ref, peak_ref, out_ref, power):
    channels, bins = out_ref.shape[3], out_ref.shape[2]
    scale = jnp.sum(peak_ref[0], axis=0) * (1.0 / TOP)
    scale = jnp.concatenate([scale[0:1], scale[1:2]], axis=1)
    power[...] = jnp.exp(jnp.log(in_ref[0].astype(jnp.float32)) * 0.125)
    for r in range(8):
        lanes = power[pl.ds(r, channels, stride=8), :].T * scale
        for m in range(128 // bins):
            out_ref[0, m * 8 + r] = lanes[m * bins : (m + 1) * bins]


def on_device(nx, ng, voltages, weights):
    v = voltages[0]
    streams, parts, channels, samples = v.shape
    rows, chans, half = streams * parts, channels // ng, samples // nx
    per = chans // CHUNKS
    group = ng // 2
    antennas = group * streams
    beams = weights.shape[3]
    own = beams // ng
    packs = own // 8
    bins = half // 8

    i = np.arange(rows * chans)[:, None]
    j = np.arange(rows * chans)[None, :]
    turn = ((j % chans == i // rows) & (j // chans == i % rows)).astype(BF16)
    i = np.arange(4 * antennas)[:, None]
    j = np.arange(2 * antennas)[None, :]
    block = i // antennas
    wants = 2 * (i % antennas) + np.where((block == 0) | (block == 3), 0, 1)
    mix = np.where(j == wants, np.where(block == 1, -1.0, 1.0), 0.0).astype(BF16)
    m = np.arange(packs)[:, None, None]
    s = np.arange(half)[None, :, None]
    lane = np.arange(128)[None, None, :]
    gather = (lane == m * bins + s // 8).astype(BF16)

    turned_weights = jnp.swapaxes(weights, 3, 4)
    vmem = pl.BlockSpec(memory_space=pltpu.VMEM)
    anywhere = pl.BlockSpec(memory_space=pl.ANY)
    packed, peaks = pl.pallas_call(
        functools.partial(kernel, nx, ng),
        out_shape=(
            jax.ShapeDtypeStruct((2, ng, CHUNKS, per * 8, 128), jnp.bfloat16),
            jax.ShapeDtypeStruct((2, group, 2, 128), jnp.float32),
        ),
        in_specs=[vmem, anywhere, vmem, vmem, vmem],
        out_specs=(anywhere, anywhere),
        scratch_shapes=[
            pltpu.VMEM((2 * CHUNKS, nx * group, per, rows, half), jnp.bfloat16),
            pltpu.VMEM((2 * CHUNKS, nx * group, per, rows, half), jnp.bfloat16),
            pltpu.VMEM(turned_weights.shape, jnp.bfloat16),
            pltpu.VMEM((ng, per, 8, 128), jnp.float32),
            pltpu.VMEM((2 * CHUNKS, ng, per * 8, 128), jnp.bfloat16),
            pltpu.VMEM((2, 128), jnp.float32),
            pltpu.SemaphoreType.DMA,
            pltpu.SemaphoreType.DMA,
            pltpu.SemaphoreType.DMA((PIECES,)),
            pltpu.SemaphoreType.DMA,
            pltpu.SemaphoreType.DMA,
            pltpu.SemaphoreType.DMA((2 * CHUNKS,)),
            pltpu.SemaphoreType.DMA((2 * CHUNKS,)),
            pltpu.SemaphoreType.DMA,
            pltpu.SemaphoreType.DMA,
            pltpu.SemaphoreType.DMA,
            pltpu.SemaphoreType.DMA,
        ],
        compiler_params=pltpu.CompilerParams(
            collective_id=0, has_side_effects=True, vmem_limit_bytes=56 * 1024 * 1024
        ),
    )(v, turned_weights, turn, mix, gather)

    spread = pl.pallas_call(
        spread_kernel,
        grid=(2,),
        out_shape=jax.ShapeDtypeStruct((2, own, bins, channels), jnp.float32),
        in_specs=[
            pl.BlockSpec((1, channels * 8, 128), lambda q: (q, 0, 0)),
            pl.BlockSpec((1, group, 2, 128), lambda q: (q, 0, 0, 0)),
        ],
        out_specs=pl.BlockSpec((1, own, bins, channels), lambda q: (q, 0, 0, 0)),
        scratch_shapes=[pltpu.VMEM((channels * 8, 128), jnp.float32)],
    )(packed.reshape(2, channels * 8, 128), peaks)
    return spread.transpose(3, 0, 1, 2)


def solution(mesh):
    nx, ng = mesh.shape["ta"], mesh.shape["gx"]

    def body(voltages, weights):
        _, streams, parts, channels, samples = voltages.shape
        rows, chans, half = streams * parts, channels // ng, samples // nx
        own = weights.shape[3] // ng
        fits = (
            nx == 2
            and rows % 16 == 0
            and chans % 16 == 0
            and half % 128 == 0
            and own % 8 == 0
            and (own // 8) * (half // 8) == 128
            and ng % 2 == 0
            and ng * chans == 256
        )
        if fits:
            return on_device(nx, ng, voltages, weights)
        return plain_on_device(voltages, weights)

    in_specs = (P("ta", "gx", None, None, None), P(None, "gx", None, None, None))
    out_specs = P(None, None, "gx", "ta")
    return jax.shard_map(
        body, mesh=mesh, in_specs=in_specs, out_specs=out_specs, check_vma=False
    )
```

```python
import functools

import jax
import jax.numpy as jnp
import numpy as np
from jax import lax
from jax.experimental import pallas as pl
from jax.experimental.pallas import tpu as pltpu
from jax.sharding import PartitionSpec as P

BF16 = np.dtype(jnp.bfloat16)
MESH = pl.DeviceIdType.MESH
CHUNKS = 4
PIECES = 4
LEAD = 6
TOP = 2.0**15.75
FLOOR = 2.0**-90
NEXT = 1.0 + 1.3 / 256


def beam_power(voltage, weight_block):
    antennas = weight_block.shape[3]
    beam_count = weight_block.shape[2]
    powers = []
    for side_index in range(2):
        real_w = weight_block[side_index, 0]
        imag_w = weight_block[side_index, 1]
        upper_rows = jnp.stack([real_w, -imag_w], axis=-1).reshape(beam_count, 2 * antennas)
        bottom_half_rows = jnp.stack([imag_w, real_w], axis=-1).reshape(beam_count, 2 * antennas)
        matrix = jnp.concatenate([upper_rows, bottom_half_rows], 0)
        signal = voltage[side_index * antennas : (side_index + 1) * antennas].reshape(
            2 * antennas, -1
        )
        beam_voltage_field = jnp.dot(matrix, signal, preferred_element_type=jnp.float32)
        power = (
            beam_voltage_field[:beam_count] * beam_voltage_field[:beam_count]
            + beam_voltage_field[beam_count:] * beam_voltage_field[beam_count:]
        )
        powers.append(power.reshape(beam_count, -1, 8).sum(-1))
    return jnp.stack(powers, 0)


def channel_powers(turned, weights):

    def one_channel(column):
        voltage = lax.dynamic_index_in_dim(turned, column, 2, keepdims=False)
        weight_block = lax.dynamic_index_in_dim(weights, column, 1, keepdims=False)
        return beam_power(voltage, weight_block)

    return lax.map(one_channel, jnp.arange(turned.shape[2], dtype=jnp.int32))


def plain_on_device(voltages, weights):
    turned = lax.all_to_all(voltages, "gx", split_axis=3, concat_axis=1, tiled=True)
    partial_power_value = channel_powers(turned[0], weights)
    relaid = lax.all_to_all(partial_power_value, "gx", split_axis=2, concat_axis=0, tiled=True)
    return lax.psum_scatter(relaid, "ta", scatter_dimension=3, tiled=True)


def kernel(
    nx, ng, v_ref, w_hbm, turn_ref, mix_ref, gather_ref, out_ref, peak_ref,
    sbuf, vrecv, w_ref, work, pbuf, peaks,
    w_sem, wsend, wz, relay_sem, wx, vsend, vget, psend, pget, msend, mget,
):
    x = lax.axis_index("ta")
    g = lax.axis_index("gx")
    me = x * ng + g
    n = nx * ng
    rows = v_ref.shape[0] * v_ref.shape[1]
    chans = v_ref.shape[2] // ng
    half = v_ref.shape[3] // nx
    per = chans // CHUNKS
    group = ng // 2
    antennas2 = group * rows
    beams = w_ref.shape[4]
    side = g // group
    u = lax.rem(g, group)
    partner = lax.rem(g + group, ng)
    steps = 2 * CHUNKS
    dests = nx * group
    mine = x * group + u
    piece = chans // nx // PIECES

    w_copy = pltpu.make_async_copy(w_hbm.at[side], w_ref.at[0], w_sem)
    w_copy.start()

    barrier = pltpu.get_barrier_semaphore()

    def greet(i, _):
        d = lax.rem(me + i, n)
        pl.semaphore_signal(
            barrier, inc=1, device_id=(d // ng, lax.rem(d, ng)), device_id_type=MESH
        )
        return 0

    lax.fori_loop(1, n, greet, 0)

    def turn_side(which):
        base = lax.rem(which + side, 2) * CHUNKS

        def turn(i, _):
            start = pl.multiple_of((which * group + i) * chans, chans)
            block = v_ref[:, :, pl.ds(start, chans), :].reshape(rows * chans, nx * half)
            turned = jnp.dot(turn_ref[...], block, preferred_element_type=jnp.float32)
            turned = turned.astype(jnp.bfloat16).reshape(CHUNKS, per, rows, nx * half)
            for k in range(nx):
                sbuf[pl.ds(base, CHUNKS), k * group + i] = turned[
                    :, :, :, k * half : (k + 1) * half
                ]
            return 0

        lax.fori_loop(0, group, turn, 0)

    def send_voltages(k):
        pltpu.make_async_copy(sbuf.at[k, mine], vrecv.at[k, mine], vget.at[k]).start()

        def send(i, _):
            d = lax.rem(mine + i, dests)
            pltpu.make_async_remote_copy(
                src_ref=sbuf.at[k, d],
                dst_ref=vrecv.at[k, mine],
                send_sem=vsend.at[k],
                recv_sem=vget.at[k],
                device_id=(d // group, side * group + lax.rem(d, group)),
                device_id_type=MESH,
            ).start()
            return 0

        lax.fori_loop(1, dests, send, 0)

    def send_weights(i):
        span = pl.ds((x * PIECES + i) * piece, piece)
        pltpu.make_async_remote_copy(
            src_ref=w_hbm.at[1 - side, span],
            dst_ref=w_ref.at[1, span],
            send_sem=wsend,
            recv_sem=wz.at[i],
            device_id=(x, partner),
            device_id_type=MESH,
        ).start()

    def relay_weights(i):
        block = w_ref.at[1, pl.ds((x * PIECES + i) * piece, piece)]
        pltpu.make_async_copy(block, block, wz.at[i]).wait()
        pltpu.make_async_remote_copy(
            src_ref=block,
            dst_ref=block,
            send_sem=relay_sem,
            recv_sem=wx,
            device_id=(1 - x, g),
            device_id_type=MESH,
        ).start()

    turn_side(side)
    pl.semaphore_wait(barrier, n - 1)
    for k in range(CHUNKS):
        send_voltages(k)
        send_weights(k)
    turn_side(1 - side)
    for k in range(CHUNKS, LEAD):
        send_voltages(k)
    w_copy.wait()

    def step(k, _):
        pltpu.make_async_copy(vrecv.at[k], vrecv.at[k], vget.at[k]).wait()

        @pl.when(k + LEAD < steps)
        def _():
            send_voltages(k + LEAD)

        @pl.when((k >= 1) & (k <= PIECES))
        def _():
            relay_weights(k - 1)

        @pl.when(k == CHUNKS)
        def _():
            other = w_ref.at[1, pl.ds((1 - x) * PIECES * piece, PIECES * piece)]
            pltpu.make_async_copy(other, other, wx).wait()

        which = k // CHUNKS
        part_of = lax.rem(k, CHUNKS)

        def channel(c, peak):
            w = w_ref[which, part_of * per + c].reshape(antennas2, beams).T
            power = None
            for h in range(nx):
                v = vrecv[k, h * group : (h + 1) * group, c].reshape(antennas2, half)
                mixed = jnp.dot(mix_ref[...], v, preferred_element_type=jnp.float32)
                mixed = mixed.astype(jnp.bfloat16)
                re = jnp.dot(w, mixed[:antennas2], preferred_element_type=jnp.float32)
                im = jnp.dot(w, mixed[antennas2:], preferred_element_type=jnp.float32)
                part = re * re + im * im
                power = part if power is None else power + part
            own = beams // ng
            packs = own // 8
            power = power.reshape(ng, packs, 8, half)
            total = None
            for m in range(packs):
                p = power[:, m].reshape(ng * 8, half)
                high = p.astype(jnp.bfloat16)
                low = (p - high.astype(jnp.float32)).astype(jnp.bfloat16)
                t = jnp.dot(high, gather_ref[m], preferred_element_type=jnp.float32)
                t += jnp.dot(low, gather_ref[m], preferred_element_type=jnp.float32)
                total = t if total is None else total + t
            total = total.reshape(ng, 8, 128)
            work[:, pl.ds(c, 1)] = total[:, None]
            return jnp.maximum(peak, jnp.max(total, axis=0))

        peak = lax.fori_loop(0, per, channel, jnp.zeros((8, 128), jnp.float32))
        peak = jnp.maximum(jnp.max(peak, keepdims=True), FLOOR)
        code = work[...].reshape(ng, per * 8, 128) * (TOP / peak)[None]
        code = code * code
        code = code * code
        code = code * code
        near = code.astype(jnp.bfloat16).astype(jnp.float32)
        pbuf[k] = jnp.where(code < near, -near, near).astype(jnp.bfloat16)
        row = lax.broadcasted_iota(jnp.int32, peaks.shape, 0)
        lane = lax.broadcasted_iota(jnp.int32, peaks.shape, 1)
        own_row = lax.rem(side + which, 2)
        first = u * chans + part_of * per
        held = (row == own_row) & (lane >= first) & (lane < first + per)
        peaks[...] = jnp.where(held, peak, peaks[...])

        target = out_ref.at[side, lax.rem(g + which * group, ng), part_of]
        pltpu.make_async_copy(pbuf.at[k, g], target, pget).start()

        def send(i, _):
            d = lax.rem(g + i, ng)
            pltpu.make_async_remote_copy(
                src_ref=pbuf.at[k, d],
                dst_ref=target,
                send_sem=psend,
                recv_sem=pget,
                device_id=(x, d),
                device_id_type=MESH,
            ).start()
            return 0

        lax.fori_loop(1, ng, send, 0)
        return 0

    peaks[...] = jnp.zeros_like(peaks)
    lax.fori_loop(0, steps, step, 0)

    pltpu.make_async_copy(peaks, peak_ref.at[side, u], mget).start()

    def send_peaks(i, _):
        pltpu.make_async_remote_copy(
            src_ref=peaks,
            dst_ref=peak_ref.at[side, u],
            send_sem=msend,
            recv_sem=mget,
            device_id=(x, lax.rem(g + i, ng)),
            device_id_type=MESH,
        ).start()
        return 0

    lax.fori_loop(1, ng, send_peaks, 0)

    pltpu.make_async_copy(peak_ref, peak_ref, mget).wait()
    pltpu.make_async_copy(out_ref, out_ref, pget).wait()
    for k in range(steps):
        sent = sbuf.at[k, pl.ds(0, dests - 1)]
        pltpu.make_async_copy(sent, sent, vsend.at[k]).wait()
    sent = pbuf.at[:, pl.ds(0, ng - 1)]
    pltpu.make_async_copy(sent, sent, psend).wait()
    sent = peak_ref.at[:, pl.ds(0, group - 1)]
    pltpu.make_async_copy(sent, sent, msend).wait()
    sent = peak_ref.at[0, pl.ds(0, 1)]
    pltpu.make_async_copy(sent, sent, msend).wait()
    sent = w_ref.at[1, pl.ds(0, PIECES * piece)]
    pltpu.make_async_copy(sent, sent, wsend).wait()
    pltpu.make_async_copy(sent, sent, relay_sem).wait()


def spread_kernel(in_ref, peak_ref, out_ref, power):
    channels, bins = out_ref.shape[3], out_ref.shape[2]
    scale = jnp.sum(peak_ref[0], axis=0) * (1.0 / TOP)
    scale = jnp.concatenate([scale[0:1], scale[1:2]], axis=1)
    code = in_ref[0].astype(jnp.float32)
    near = jnp.abs(code)
    gap = (near * NEXT).astype(jnp.bfloat16).astype(jnp.float32) - near
    near = near + jnp.where(code < 0, -0.25, 0.25) * gap
    power[...] = jnp.exp(jnp.log(near) * 0.125)
    for r in range(8):
        lanes = power[pl.ds(r, channels, stride=8), :].T * scale
        for m in range(128 // bins):
            out_ref[0, m * 8 + r] = lanes[m * bins : (m + 1) * bins]


def on_device(nx, ng, voltages, weights):
    v = voltages[0]
    streams, parts, channels, samples = v.shape
    rows, chans, half = streams * parts, channels // ng, samples // nx
    per = chans // CHUNKS
    group = ng // 2
    antennas = group * streams
    beams = weights.shape[3]
    own = beams // ng
    packs = own // 8
    bins = half // 8

    i = np.arange(rows * chans)[:, None]
    j = np.arange(rows * chans)[None, :]
    turn = ((j % chans == i // rows) & (j // chans == i % rows)).astype(BF16)
    i = np.arange(4 * antennas)[:, None]
    j = np.arange(2 * antennas)[None, :]
    block = i // antennas
    wants = 2 * (i % antennas) + np.where((block == 0) | (block == 3), 0, 1)
    mix = np.where(j == wants, np.where(block == 1, -1.0, 1.0), 0.0).astype(BF16)
    m = np.arange(packs)[:, None, None]
    s = np.arange(half)[None, :, None]
    lane = np.arange(128)[None, None, :]
    gather = (lane == m * bins + s // 8).astype(BF16)

    turned_weights = jnp.swapaxes(weights, 3, 4)
    vmem = pl.BlockSpec(memory_space=pltpu.VMEM)
    anywhere = pl.BlockSpec(memory_space=pl.ANY)
    packed, peaks = pl.pallas_call(
        functools.partial(kernel, nx, ng),
        out_shape=(
            jax.ShapeDtypeStruct((2, ng, CHUNKS, per * 8, 128), jnp.bfloat16),
            jax.ShapeDtypeStruct((2, group, 2, 128), jnp.float32),
        ),
        in_specs=[vmem, anywhere, vmem, vmem, vmem],
        out_specs=(anywhere, anywhere),
        scratch_shapes=[
            pltpu.VMEM((2 * CHUNKS, nx * group, per, rows, half), jnp.bfloat16),
            pltpu.VMEM((2 * CHUNKS, nx * group, per, rows, half), jnp.bfloat16),
            pltpu.VMEM(turned_weights.shape, jnp.bfloat16),
            pltpu.VMEM((ng, per, 8, 128), jnp.float32),
            pltpu.VMEM((2 * CHUNKS, ng, per * 8, 128), jnp.bfloat16),
            pltpu.VMEM((2, 128), jnp.float32),
            pltpu.SemaphoreType.DMA,
            pltpu.SemaphoreType.DMA,
            pltpu.SemaphoreType.DMA((PIECES,)),
            pltpu.SemaphoreType.DMA,
            pltpu.SemaphoreType.DMA,
            pltpu.SemaphoreType.DMA((2 * CHUNKS,)),
            pltpu.SemaphoreType.DMA((2 * CHUNKS,)),
            pltpu.SemaphoreType.DMA,
            pltpu.SemaphoreType.DMA,
            pltpu.SemaphoreType.DMA,
            pltpu.SemaphoreType.DMA,
        ],
        compiler_params=pltpu.CompilerParams(
            collective_id=0, has_side_effects=True, vmem_limit_bytes=56 * 1024 * 1024
        ),
    )(v, turned_weights, turn, mix, gather)

    spread = pl.pallas_call(
        spread_kernel,
        grid=(2,),
        out_shape=jax.ShapeDtypeStruct((2, own, bins, channels), jnp.float32),
        in_specs=[
            pl.BlockSpec((1, channels * 8, 128), lambda q: (q, 0, 0)),
            pl.BlockSpec((1, group, 2, 128), lambda q: (q, 0, 0, 0)),
        ],
        out_specs=pl.BlockSpec((1, own, bins, channels), lambda q: (q, 0, 0, 0)),
        scratch_shapes=[pltpu.VMEM((channels * 8, 128), jnp.float32)],
    )(packed.reshape(2, channels * 8, 128), peaks)
    return spread.transpose(3, 0, 1, 2)


def solution(mesh):
    nx, ng = mesh.shape["ta"], mesh.shape["gx"]

    def body(voltages, weights):
        _, streams, parts, channels, samples = voltages.shape
        rows, chans, half = streams * parts, channels // ng, samples // nx
        own = weights.shape[3] // ng
        fits = (
            nx == 2
            and rows % 16 == 0
            and chans % 16 == 0
            and half % 128 == 0
            and own % 8 == 0
            and (own // 8) * (half // 8) == 128
            and ng % 2 == 0
            and ng * chans == 256
        )
        if fits:
            return on_device(nx, ng, voltages, weights)
        return plain_on_device(voltages, weights)

    in_specs = (P("ta", "gx", None, None, None), P(None, "gx", None, None, None))
    out_specs = P(None, None, "gx", "ta")
    return jax.shard_map(
        body, mesh=mesh, in_specs=in_specs, out_specs=out_specs, check_vma=False
    )
```

```python
import functools

import jax
import jax.numpy as jnp
from jax import lax
from jax.experimental import pallas as pl
from jax.experimental.pallas import tpu as pltpu
from jax.sharding import PartitionSpec as P

MESH = pl.DeviceIdType.MESH
VMEM = 61 * 1024 * 1024
CHUNKS = 4
PIECES = 4
HOLD = 2
LEAD = 6
TOP = 2.0**15.75
FLOOR = 2.0**-90
NEXT = 1.0 + 1.3 / 256


def beam_power(voltage, weight_block):
    antennas = weight_block.shape[3]
    beam_count = weight_block.shape[2]
    powers = []
    for side_index in range(2):
        real_w = weight_block[side_index, 0]
        imag_w = weight_block[side_index, 1]
        upper_rows = jnp.stack([real_w, -imag_w], axis=-1).reshape(beam_count, 2 * antennas)
        bottom_half_rows = jnp.stack([imag_w, real_w], axis=-1).reshape(beam_count, 2 * antennas)
        matrix = jnp.concatenate([upper_rows, bottom_half_rows], 0)
        signal = voltage[side_index * antennas : (side_index + 1) * antennas].reshape(
            2 * antennas, -1
        )
        beam_voltage_field = jnp.dot(matrix, signal, preferred_element_type=jnp.float32)
        power = (
            beam_voltage_field[:beam_count] * beam_voltage_field[:beam_count]
            + beam_voltage_field[beam_count:] * beam_voltage_field[beam_count:]
        )
        powers.append(power.reshape(beam_count, -1, 8).sum(-1))
    return jnp.stack(powers, 0)


def channel_powers(turned, weights):

    def one_channel(column):
        voltage = lax.dynamic_index_in_dim(turned, column, 2, keepdims=False)
        weight_block = lax.dynamic_index_in_dim(weights, column, 1, keepdims=False)
        return beam_power(voltage, weight_block)

    return lax.map(one_channel, jnp.arange(turned.shape[2], dtype=jnp.int32))


def plain_on_device(voltages, weights):
    turned = lax.all_to_all(voltages, "gx", split_axis=3, concat_axis=1, tiled=True)
    partial_power_value = channel_powers(turned[0], weights)
    relaid = lax.all_to_all(partial_power_value, "gx", split_axis=2, concat_axis=0, tiled=True)
    return lax.psum_scatter(relaid, "ta", scatter_dimension=3, tiled=True)


def kernel(
    nx, ng, v_hbm, w_hbm, out_ref, peak_ref,
    turn_ref, mix_ref, gather_ref, vbuf, sbuf, vrecv, w_ref, work, pbuf, peaks,
    v_sem, cross, w_sem, wsend, wz, relay_sem, wx, vsend, vget, psend, pget, msend, mget,
):
    x = lax.axis_index("ta")
    g = lax.axis_index("gx")
    rows = v_hbm.shape[0] * v_hbm.shape[1]
    chans = v_hbm.shape[2] // ng
    half = v_hbm.shape[3] // nx
    per = chans // CHUNKS
    group = ng // 2
    antennas2 = group * rows
    beams = w_ref.shape[4]
    side = g // group
    u = lax.rem(g, group)
    partner = lax.rem(g + group, ng)
    steps = 2 * CHUNKS
    dests = nx * group
    mine = x * group + u
    piece = chans // nx // PIECES

    barrier = pltpu.get_barrier_semaphore()

    def greet(i, _):
        d = mine ^ i
        pl.semaphore_signal(
            barrier,
            inc=1,
            device_id=(d // group, side * group + lax.rem(d, group)),
            device_id_type=MESH,
        )
        return 0

    lax.fori_loop(1, dests, greet, 0)
    pl.semaphore_signal(barrier, inc=1, device_id=(x, partner), device_id_type=MESH)

    w_copy = pltpu.make_async_copy(w_hbm.at[side], w_ref.at[0], w_sem)

    def fetch(block):
        return pltpu.make_async_copy(
            v_hbm.at[:, :, pl.ds(pl.multiple_of(block * chans, chans), chans), :],
            vbuf.at[block],
            v_sem.at[block],
        )

    def fetch_side(which):
        def start(i, _):
            fetch(which * group + i).start()
            return 0

        lax.fori_loop(0, group, start, 0)

    fetch_side(side)
    fetch_side(1 - side)
    w_copy.start()

    def grid_of(shape):
        return [lax.broadcasted_iota(jnp.int32, shape, axis) for axis in (0, 1)]

    i, j = grid_of(turn_ref.shape)
    hit = (j % chans == i // rows) & (j // chans == i % rows)
    turn_ref[...] = hit.astype(jnp.float32).astype(jnp.bfloat16)

    def turn_side(which):
        base = lax.rem(which + side, 2) * CHUNKS

        def turn(i, _):
            fetch(which * group + i).wait()
            block = vbuf[which * group + i].reshape(rows * chans, nx * half)
            turned = jnp.dot(turn_ref[...], block, preferred_element_type=jnp.float32)
            turned = turned.astype(jnp.bfloat16).reshape(CHUNKS, per, rows, nx * half)
            for k in range(nx):
                sbuf[pl.ds(base, CHUNKS), k * group + i] = turned[
                    :, :, :, k * half : (k + 1) * half
                ]
            return 0

        lax.fori_loop(0, group, turn, 0)

    def send_voltages(k):
        first = k // CHUNKS * CHUNKS
        skew = k // CHUNKS * (CHUNKS // nx)

        def source(d):
            return sbuf.at[first + lax.rem(k - first + d // group * skew, CHUNKS), d]

        pltpu.make_async_copy(source(mine), vrecv.at[k, mine], vget.at[k]).start()

        def send(i, _):
            d = mine ^ (dests - i)
            pltpu.make_async_remote_copy(
                src_ref=source(d),
                dst_ref=vrecv.at[k, mine],
                send_sem=vsend.at[k],
                recv_sem=vget.at[k],
                device_id=(d // group, side * group + lax.rem(d, group)),
                device_id_type=MESH,
            ).start()
            return 0

        lax.fori_loop(1, dests, send, 0)

    def send_weights(i):
        span = pl.ds((x * PIECES + i) * piece, piece)
        pltpu.make_async_remote_copy(
            src_ref=w_hbm.at[1 - side, span],
            dst_ref=w_ref.at[1, span],
            send_sem=wsend,
            recv_sem=wz.at[i],
            device_id=(x, partner),
            device_id_type=MESH,
        ).start()

    def relay_weights(i):
        block = w_ref.at[1, pl.ds((x * PIECES + i) * piece, piece)]
        pltpu.make_async_copy(block, block, wz.at[i]).wait()
        pltpu.make_async_remote_copy(
            src_ref=block,
            dst_ref=block,
            send_sem=relay_sem,
            recv_sem=wx.at[i],
            device_id=(1 - x, g),
            device_id_type=MESH,
        ).start()

    turn_side(side)
    pl.semaphore_wait(barrier, dests)
    pl.semaphore_signal(cross, inc=1, device_id=(x, partner), device_id_type=MESH)
    for k in range(CHUNKS):
        send_voltages(k)
        send_weights(k)
    turn_side(1 - side)
    for k in range(CHUNKS, LEAD):
        send_voltages(k)
    antennas = antennas2 // 2
    i, j = grid_of(mix_ref.shape)
    block = i // antennas
    wants = 2 * (i % antennas) + ((block == 1) | (block == 2)).astype(jnp.int32)
    sign = jnp.where(block == 1, -1.0, 1.0)
    mix_ref[...] = jnp.where(j == wants, sign, 0.0).astype(jnp.bfloat16)
    sample, lane = grid_of(gather_ref.shape[1:])
    for m in range(gather_ref.shape[0]):
        hit = lane == m * (half // 8) + sample // 8
        gather_ref[m] = hit.astype(jnp.float32).astype(jnp.bfloat16)
    w_copy.wait()

    def step(k, _):
        pltpu.make_async_copy(vrecv.at[k], vrecv.at[k], vget.at[k]).wait()

        @pl.when(k + LEAD < steps)
        def _():
            send_voltages(k + LEAD)

        @pl.when((k >= HOLD) & (k < HOLD + PIECES))
        def _():
            relay_weights(k - HOLD)

        for i in range(PIECES):

            @pl.when(k == steps - CHUNKS // nx + i * CHUNKS // nx // PIECES)
            def _(i=i):
                other = w_ref.at[1, pl.ds(((1 - x) * PIECES + i) * piece, piece)]
                pltpu.make_async_copy(other, other, wx.at[i]).wait()

        which = k // CHUNKS
        part_of = lax.rem(k + which * x * (CHUNKS // nx), CHUNKS)

        def channel(c, peak):
            w = w_ref[which, part_of * per + c].reshape(antennas2, beams).T
            power = None
            for h in range(nx):
                v = vrecv[k, h * group : (h + 1) * group, c].reshape(antennas2, half)
                mixed = jnp.dot(mix_ref[...], v, preferred_element_type=jnp.float32)
                mixed = mixed.astype(jnp.bfloat16)
                re = jnp.dot(w, mixed[:antennas2], preferred_element_type=jnp.float32)
                im = jnp.dot(w, mixed[antennas2:], preferred_element_type=jnp.float32)
                part = re * re + im * im
                power = part if power is None else power + part
            own = beams // ng
            packs = own // 8
            power = power.reshape(ng, packs, 8, half)
            total = None
            for m in range(packs):
                p = power[:, m].reshape(ng * 8, half)
                high = p.astype(jnp.bfloat16)
                low = (p - high.astype(jnp.float32)).astype(jnp.bfloat16)
                t = jnp.dot(high, gather_ref[m], preferred_element_type=jnp.float32)
                t += jnp.dot(low, gather_ref[m], preferred_element_type=jnp.float32)
                total = t if total is None else total + t
            total = total.reshape(ng, 8, 128)
            work[:, pl.ds(c, 1)] = total[:, None]
            return jnp.maximum(peak, jnp.max(total, axis=0))

        peak = lax.fori_loop(0, per, channel, jnp.zeros((8, 128), jnp.float32))
        peak = jnp.maximum(jnp.max(peak, keepdims=True), FLOOR)
        code = work[...].reshape(ng, per * 8, 128) * (TOP / peak)[None]
        code = code * code
        code = code * code
        code = code * code
        near = code.astype(jnp.bfloat16).astype(jnp.float32)
        pbuf[k] = jnp.where(code < near, -near, near).astype(jnp.bfloat16)
        row = lax.broadcasted_iota(jnp.int32, peaks.shape, 0)
        lane = lax.broadcasted_iota(jnp.int32, peaks.shape, 1)
        own_row = lax.rem(side + which, 2)
        first = u * chans + part_of * per
        held = (row == own_row) & (lane >= first) & (lane < first + per)
        peaks[...] = jnp.where(held, peak, peaks[...])

        @pl.when(k == 0)
        def _():
            pl.semaphore_wait(cross, 1)

        target = out_ref.at[side, lax.rem(g + which * group, ng), part_of]
        pltpu.make_async_copy(pbuf.at[k, g], target, pget).start()

        def send(i, _):
            d = g ^ (ng - i)
            pltpu.make_async_remote_copy(
                src_ref=pbuf.at[k, d],
                dst_ref=target,
                send_sem=psend,
                recv_sem=pget,
                device_id=(x, d),
                device_id_type=MESH,
            ).start()
            return 0

        lax.fori_loop(1, ng, send, 0)
        return 0

    peaks[...] = jnp.zeros_like(peaks)
    lax.fori_loop(0, steps, step, 0)

    pltpu.make_async_copy(peaks, peak_ref.at[side, u], mget).start()

    def send_peaks(i, _):
        pltpu.make_async_remote_copy(
            src_ref=peaks,
            dst_ref=peak_ref.at[side, u],
            send_sem=msend,
            recv_sem=mget,
            device_id=(x, lax.rem(g + i, ng)),
            device_id_type=MESH,
        ).start()
        return 0

    lax.fori_loop(1, ng, send_peaks, 0)

    pltpu.make_async_copy(peak_ref, peak_ref, mget).wait()
    pltpu.make_async_copy(out_ref, out_ref, pget).wait()
    for k in range(steps):
        sent = sbuf.at[k, pl.ds(0, dests - 1)]
        pltpu.make_async_copy(sent, sent, vsend.at[k]).wait()
    sent = pbuf.at[:, pl.ds(0, ng - 1)]
    pltpu.make_async_copy(sent, sent, psend).wait()
    sent = peak_ref.at[:, pl.ds(0, group - 1)]
    pltpu.make_async_copy(sent, sent, msend).wait()
    sent = peak_ref.at[0, pl.ds(0, 1)]
    pltpu.make_async_copy(sent, sent, msend).wait()
    sent = w_ref.at[1, pl.ds(0, PIECES * piece)]
    pltpu.make_async_copy(sent, sent, wsend).wait()
    pltpu.make_async_copy(sent, sent, relay_sem).wait()


def spread_kernel(in_ref, peak_ref, out_ref, power):
    channels, bins = out_ref.shape[3], out_ref.shape[2]
    scale = jnp.sum(peak_ref[0], axis=0) * (1.0 / TOP)
    scale = jnp.concatenate([scale[0:1], scale[1:2]], axis=1)
    code = in_ref[0].astype(jnp.float32)
    near = jnp.abs(code)
    gap = (near * NEXT).astype(jnp.bfloat16).astype(jnp.float32) - near
    near = near + jnp.where(code < 0, -0.25, 0.25) * gap
    power[...] = jnp.exp(jnp.log(near) * 0.125)
    for r in range(8):
        lanes = power[pl.ds(r, channels, stride=8), :].T * scale
        for m in range(128 // bins):
            out_ref[0, m * 8 + r] = lanes[m * bins : (m + 1) * bins]


def on_device(nx, ng, voltages, weights):
    v = voltages[0]
    streams, parts, channels, samples = v.shape
    rows, chans, half = streams * parts, channels // ng, samples // nx
    per = chans // CHUNKS
    group = ng // 2
    antennas = group * streams
    beams = weights.shape[3]
    own = beams // ng
    packs = own // 8
    bins = half // 8

    turned_weights = jnp.swapaxes(weights, 3, 4)
    hbm = pl.BlockSpec(memory_space=pltpu.HBM)
    anywhere = pl.BlockSpec(memory_space=pl.ANY)
    packed, peaks = pl.pallas_call(
        functools.partial(kernel, nx, ng),
        out_shape=(
            jax.ShapeDtypeStruct((2, ng, CHUNKS, per * 8, 128), jnp.bfloat16),
            jax.ShapeDtypeStruct((2, group, 2, 128), jnp.float32),
        ),
        in_specs=[hbm, hbm],
        out_specs=(anywhere, anywhere),
        scratch_shapes=[
            pltpu.VMEM((rows * chans, rows * chans), jnp.bfloat16),
            pltpu.VMEM((4 * antennas, 2 * antennas), jnp.bfloat16),
            pltpu.VMEM((packs, half, 128), jnp.bfloat16),
            pltpu.VMEM((2 * group, streams, parts, chans, samples), jnp.bfloat16),
            pltpu.VMEM((2 * CHUNKS, nx * group, per, rows, half), jnp.bfloat16),
            pltpu.VMEM((2 * CHUNKS, nx * group, per, rows, half), jnp.bfloat16),
            pltpu.VMEM(turned_weights.shape, jnp.bfloat16),
            pltpu.VMEM((ng, per, 8, 128), jnp.float32),
            pltpu.VMEM((2 * CHUNKS, ng, per * 8, 128), jnp.bfloat16),
            pltpu.VMEM((2, 128), jnp.float32),
            pltpu.SemaphoreType.DMA((2 * group,)),
            pltpu.SemaphoreType.REGULAR,
            pltpu.SemaphoreType.DMA,
            pltpu.SemaphoreType.DMA,
            pltpu.SemaphoreType.DMA((PIECES,)),
            pltpu.SemaphoreType.DMA,
            pltpu.SemaphoreType.DMA((PIECES,)),
            pltpu.SemaphoreType.DMA((2 * CHUNKS,)),
            pltpu.SemaphoreType.DMA((2 * CHUNKS,)),
            pltpu.SemaphoreType.DMA,
            pltpu.SemaphoreType.DMA,
            pltpu.SemaphoreType.DMA,
            pltpu.SemaphoreType.DMA,
        ],
        compiler_params=pltpu.CompilerParams(
            collective_id=0, has_side_effects=True, vmem_limit_bytes=VMEM
        ),
    )(v, turned_weights)

    spread = pl.pallas_call(
        spread_kernel,
        grid=(2,),
        out_shape=jax.ShapeDtypeStruct((2, own, bins, channels), jnp.float32),
        in_specs=[
            pl.BlockSpec((1, channels * 8, 128), lambda q: (q, 0, 0)),
            pl.BlockSpec((1, group, 2, 128), lambda q: (q, 0, 0, 0)),
        ],
        out_specs=pl.BlockSpec((1, own, bins, channels), lambda q: (q, 0, 0, 0)),
        scratch_shapes=[pltpu.VMEM((channels * 8, 128), jnp.float32)],
        compiler_params=pltpu.CompilerParams(vmem_limit_bytes=VMEM),
    )(packed.reshape(2, channels * 8, 128), peaks)
    return spread.transpose(3, 0, 1, 2)


def solution(mesh):
    nx, ng = mesh.shape["ta"], mesh.shape["gx"]

    def body(voltages, weights):
        _, streams, parts, channels, samples = voltages.shape
        rows, chans, half = streams * parts, channels // ng, samples // nx
        own = weights.shape[3] // ng
        fits = (
            nx == 2
            and rows % 16 == 0
            and chans % 16 == 0
            and half % 128 == 0
            and own % 8 == 0
            and (own // 8) * (half // 8) == 128
            and ng % 2 == 0
            and ng & (ng - 1) == 0
            and ng * chans == 256
        )
        if fits:
            return on_device(nx, ng, voltages, weights)
        return plain_on_device(voltages, weights)

    in_specs = (P("ta", "gx", None, None, None), P(None, "gx", None, None, None))
    out_specs = P(None, None, "gx", "ta")
    return jax.shard_map(
        body, mesh=mesh, in_specs=in_specs, out_specs=out_specs, check_vma=False
    )
```

```python
import functools

import jax
import jax.numpy as jnp
from jax import lax
from jax.experimental import pallas as pl
from jax.experimental.pallas import tpu as pltpu
from jax.sharding import PartitionSpec as P

MESH = pl.DeviceIdType.MESH
VMEM = 48 * 1024 * 1024
CHUNKS = 4
PIECES = 4
HOLD = 2
LEAD = 8
TOP = 2.0**15.75
FLOOR = 2.0**-90
NEXT = 1.0 + 1.3 / 256


def beam_power(voltage, weight_block):
    antennas = weight_block.shape[3]
    beam_count = weight_block.shape[2]
    powers = []
    for side_index in range(2):
        real_w = weight_block[side_index, 0]
        imag_w = weight_block[side_index, 1]
        upper_rows = jnp.stack([real_w, -imag_w], axis=-1).reshape(beam_count, 2 * antennas)
        bottom_half_rows = jnp.stack([imag_w, real_w], axis=-1).reshape(beam_count, 2 * antennas)
        matrix = jnp.concatenate([upper_rows, bottom_half_rows], 0)
        signal = voltage[side_index * antennas : (side_index + 1) * antennas].reshape(
            2 * antennas, -1
        )
        beam_voltage_field = jnp.dot(matrix, signal, preferred_element_type=jnp.float32)
        power = (
            beam_voltage_field[:beam_count] * beam_voltage_field[:beam_count]
            + beam_voltage_field[beam_count:] * beam_voltage_field[beam_count:]
        )
        powers.append(power.reshape(beam_count, -1, 8).sum(-1))
    return jnp.stack(powers, 0)


def channel_powers(turned, weights):

    def one_channel(column):
        voltage = lax.dynamic_index_in_dim(turned, column, 2, keepdims=False)
        weight_block = lax.dynamic_index_in_dim(weights, column, 1, keepdims=False)
        return beam_power(voltage, weight_block)

    return lax.map(one_channel, jnp.arange(turned.shape[2], dtype=jnp.int32))


def plain_on_device(voltages, weights):
    turned = lax.all_to_all(voltages, "gx", split_axis=3, concat_axis=1, tiled=True)
    partial_power_value = channel_powers(turned[0], weights)
    relaid = lax.all_to_all(partial_power_value, "gx", split_axis=2, concat_axis=0, tiled=True)
    return lax.psum_scatter(relaid, "ta", scatter_dimension=3, tiled=True)


def kernel(
    nx, ng, v_hbm, w_hbm, out_ref, peak_ref,
    turn_ref, mix_ref, gather_ref, vbuf, sbuf, vrecv, w_ref, work, pbuf, codes, plain, peaks,
    v_sem, cross, w_sem, wsend, wz, relay_sem, wx, vsend, vget, psend, pget, msend, mget, out_sem,
):
    x = lax.axis_index("ta")
    g = lax.axis_index("gx")
    rows = v_hbm.shape[0] * v_hbm.shape[1]
    chans = v_hbm.shape[2] // ng
    half = v_hbm.shape[3] // nx
    per = chans // CHUNKS
    group = ng // 2
    antennas2 = group * rows
    beams = w_ref.shape[4]
    side = g // group
    u = lax.rem(g, group)
    partner = lax.rem(g + group, ng)
    steps = 2 * CHUNKS
    dests = nx * group
    mine = x * group + u
    piece = chans // nx // PIECES

    barrier = pltpu.get_barrier_semaphore()

    def greet(i, _):
        d = mine ^ i
        pl.semaphore_signal(
            barrier,
            inc=1,
            device_id=(d // group, side * group + lax.rem(d, group)),
            device_id_type=MESH,
        )
        return 0

    lax.fori_loop(1, dests, greet, 0)
    pl.semaphore_signal(barrier, inc=1, device_id=(x, partner), device_id_type=MESH)

    w_copy = pltpu.make_async_copy(w_hbm.at[side], w_ref.at[0], w_sem)

    def fetch(block):
        return pltpu.make_async_copy(
            v_hbm.at[:, :, pl.ds(pl.multiple_of(block * chans, chans), chans), :],
            vbuf.at[block],
            v_sem.at[block],
        )

    def fetch_side(which):
        def start(i, _):
            fetch(which * group + (u ^ (group - 1 - i))).start()
            return 0

        lax.fori_loop(0, group, start, 0)

    fetch_side(side)
    fetch_side(1 - side)
    w_copy.start()

    def grid_of(shape):
        return [lax.broadcasted_iota(jnp.int32, shape, axis) for axis in (0, 1)]

    i, j = grid_of(turn_ref.shape)
    hit = (j % chans == i // rows) & (j // chans == i % rows)
    turn_ref[...] = hit.astype(jnp.float32).astype(jnp.bfloat16)

    def turn_block(which, b):
        base = lax.rem(which + side, 2) * CHUNKS
        fetch(which * group + b).wait()
        block = vbuf[which * group + b].reshape(rows * chans, nx * half)
        turned = jnp.dot(turn_ref[...], block, preferred_element_type=jnp.float32)
        turned = turned.astype(jnp.bfloat16).reshape(CHUNKS, per, rows, nx * half)
        for k in range(nx):
            sbuf[pl.ds(base, CHUNKS), k * group + b] = turned[
                :, :, :, k * half : (k + 1) * half
            ]

    def send_voltage(k, d):
        first = k // CHUNKS * CHUNKS
        skew = k // CHUNKS * (CHUNKS // nx)
        return pltpu.make_async_remote_copy(
            src_ref=sbuf.at[first + lax.rem(k - first + d // group * skew, CHUNKS), d],
            dst_ref=vrecv.at[k, mine],
            send_sem=vsend.at[k],
            recv_sem=vget.at[k],
            device_id=(d // group, side * group + lax.rem(d, group)),
            device_id_type=MESH,
        )

    def keep_voltages(k):
        first = k // CHUNKS * CHUNKS
        skew = k // CHUNKS * (CHUNKS // nx)
        own = sbuf.at[first + lax.rem(k - first + x * skew, CHUNKS), mine]
        pltpu.make_async_copy(own, vrecv.at[k, mine], vget.at[k]).start()

    def send_voltages(k):
        keep_voltages(k)

        def send(i, _):
            send_voltage(k, mine ^ (dests - i)).start()
            return 0

        lax.fori_loop(1, dests, send, 0)

    def send_weights(i):
        span = pl.ds((x * PIECES + i) * piece, piece)
        pltpu.make_async_remote_copy(
            src_ref=w_hbm.at[1 - side, span],
            dst_ref=w_ref.at[1, span],
            send_sem=wsend,
            recv_sem=wz.at[i],
            device_id=(x, partner),
            device_id_type=MESH,
        ).start()

    def relay_weights(i):
        block = w_ref.at[1, pl.ds((x * PIECES + i) * piece, piece)]
        pltpu.make_async_copy(block, block, wz.at[i]).wait()
        pltpu.make_async_remote_copy(
            src_ref=block,
            dst_ref=block,
            send_sem=relay_sem,
            recv_sem=wx.at[i],
            device_id=(1 - x, g),
            device_id_type=MESH,
        ).start()

    pl.semaphore_wait(barrier, dests)
    pl.semaphore_signal(cross, inc=1, device_id=(x, partner), device_id_type=MESH)

    def turn_and_send(i, _):
        @pl.when(i > 0)
        def _():
            b = u ^ (group - i)
            send_voltage(0, (1 - x) * group + b).start()
            send_voltage(0, x * group + b).start()

        turn_block(side, u ^ (group - 1 - i))
        return 0

    lax.fori_loop(0, group, turn_and_send, 0)
    send_weights(0)
    send_voltage(0, (1 - x) * group + u).start()
    keep_voltages(0)
    for k in range(1, CHUNKS):
        send_voltages(k)
        send_weights(k)

    def turn(i, _):
        turn_block(1 - side, i)
        return 0

    lax.fori_loop(0, group, turn, 0)
    for k in range(CHUNKS, LEAD):
        send_voltages(k)
    antennas = antennas2 // 2
    i, j = grid_of(mix_ref.shape)
    block = i // antennas
    wants = 2 * (i % antennas) + ((block == 1) | (block == 2)).astype(jnp.int32)
    sign = jnp.where(block == 1, -1.0, 1.0)
    mix_ref[...] = jnp.where(j == wants, sign, 0.0).astype(jnp.bfloat16)
    sample, lane = grid_of(gather_ref.shape[1:])
    for m in range(gather_ref.shape[0]):
        hit = lane == m * (half // 8) + sample // 8
        gather_ref[m] = hit.astype(jnp.float32).astype(jnp.bfloat16)
    w_copy.wait()

    def step(k, _):
        pltpu.make_async_copy(vrecv.at[k], vrecv.at[k], vget.at[k]).wait()

        @pl.when(k + LEAD < steps)
        def _():
            send_voltages(k + LEAD)

        @pl.when((k >= HOLD) & (k < HOLD + PIECES))
        def _():
            relay_weights(k - HOLD)

        for i in range(PIECES):

            @pl.when(k == steps - CHUNKS // nx + i * CHUNKS // nx // PIECES)
            def _(i=i):
                other = w_ref.at[1, pl.ds(((1 - x) * PIECES + i) * piece, piece)]
                pltpu.make_async_copy(other, other, wx.at[i]).wait()

        which = k // CHUNKS
        part_of = lax.rem(k + which * x * (CHUNKS // nx), CHUNKS)

        def channel(c, peak):
            w = w_ref[which, part_of * per + c].reshape(antennas2, beams).T
            power = None
            for h in range(nx):
                v = vrecv[k, h * group : (h + 1) * group, c].reshape(antennas2, half)
                mixed = jnp.dot(mix_ref[...], v, preferred_element_type=jnp.float32)
                mixed = mixed.astype(jnp.bfloat16)
                re = jnp.dot(w, mixed[:antennas2], preferred_element_type=jnp.float32)
                im = jnp.dot(w, mixed[antennas2:], preferred_element_type=jnp.float32)
                part = re * re + im * im
                power = part if power is None else power + part
            own = beams // ng
            packs = own // 8
            power = power.reshape(ng, packs, 8, half)
            total = None
            for m in range(packs):
                p = power[:, m].reshape(ng * 8, half)
                high = p.astype(jnp.bfloat16)
                low = (p - high.astype(jnp.float32)).astype(jnp.bfloat16)
                t = jnp.dot(high, gather_ref[m], preferred_element_type=jnp.float32)
                t += jnp.dot(low, gather_ref[m], preferred_element_type=jnp.float32)
                total = t if total is None else total + t
            total = total.reshape(ng, 8, 128)
            work[:, pl.ds(c, 1)] = total[:, None]
            return jnp.maximum(peak, jnp.max(total, axis=0))

        peak = lax.fori_loop(0, per, channel, jnp.zeros((8, 128), jnp.float32))
        peak = jnp.maximum(jnp.max(peak, keepdims=True), FLOOR)
        code = work[...].reshape(ng, per * 8, 128) * (TOP / peak)[None]
        code = code * code
        code = code * code
        code = code * code
        near = code.astype(jnp.bfloat16).astype(jnp.float32)
        pbuf[k] = jnp.where(code < near, -near, near).astype(jnp.bfloat16)
        row = lax.broadcasted_iota(jnp.int32, peaks.shape, 0)
        lane = lax.broadcasted_iota(jnp.int32, peaks.shape, 1)
        own_row = lax.rem(side + which, 2)
        first = u * chans + part_of * per
        held = (row == own_row) & (lane >= first) & (lane < first + per)
        peaks[...] = jnp.where(held, peak, peaks[...])

        @pl.when(k == 0)
        def _():
            pl.semaphore_wait(cross, 1)

        target = codes.at[side, lax.rem(g + which * group, ng), part_of]
        pltpu.make_async_copy(pbuf.at[k, g], target, pget.at[k]).start()

        def send(i, _):
            d = g ^ (ng - i)
            pltpu.make_async_remote_copy(
                src_ref=pbuf.at[k, d],
                dst_ref=target,
                send_sem=psend,
                recv_sem=pget.at[k],
                device_id=(x, d),
                device_id_type=MESH,
            ).start()
            return 0

        lax.fori_loop(1, ng, send, 0)
        return 0

    peaks[...] = jnp.zeros_like(peaks)
    lax.fori_loop(0, steps, step, 0)

    pltpu.make_async_copy(peaks, peak_ref.at[side, u], mget).start()

    def send_peaks(i, _):
        pltpu.make_async_remote_copy(
            src_ref=peaks,
            dst_ref=peak_ref.at[side, u],
            send_sem=msend,
            recv_sem=mget,
            device_id=(x, lax.rem(g + i, ng)),
            device_id_type=MESH,
        ).start()
        return 0

    lax.fori_loop(1, ng, send_peaks, 0)

    def decode(k, _):
        pltpu.make_async_copy(pbuf.at[k], pbuf.at[k], pget.at[k]).wait()
        which = k // CHUNKS
        part_of = lax.rem(k + which * x * (CHUNKS // nx), CHUNKS)
        for other in range(2):
            span = pl.ds((other + which) % 2 * group, group)
            code = codes[other, span, part_of].astype(jnp.float32)
            near = jnp.abs(code)
            gap = (near * NEXT).astype(jnp.bfloat16).astype(jnp.float32) - near
            near = near + jnp.where(code < 0, -0.25, 0.25) * gap
            plain[other, span, part_of] = jnp.exp(jnp.log(near) * 0.125)
            pltpu.make_async_copy(
                plain.at[other, span, part_of],
                out_ref.at[other, span, part_of],
                out_sem,
            ).start()
        return 0

    lax.fori_loop(0, steps, decode, 0)
    pltpu.make_async_copy(peak_ref, peak_ref, mget).wait()
    pltpu.make_async_copy(out_ref, out_ref, out_sem).wait()
    for k in range(steps):
        sent = sbuf.at[k, pl.ds(0, dests - 1)]
        pltpu.make_async_copy(sent, sent, vsend.at[k]).wait()
    sent = pbuf.at[:, pl.ds(0, ng - 1)]
    pltpu.make_async_copy(sent, sent, psend).wait()
    sent = peak_ref.at[:, pl.ds(0, group - 1)]
    pltpu.make_async_copy(sent, sent, msend).wait()
    sent = peak_ref.at[0, pl.ds(0, 1)]
    pltpu.make_async_copy(sent, sent, msend).wait()
    sent = w_ref.at[1, pl.ds(0, PIECES * piece)]
    pltpu.make_async_copy(sent, sent, wsend).wait()
    pltpu.make_async_copy(sent, sent, relay_sem).wait()


def spread_kernel(in_ref, peak_ref, out_ref):
    channels, bins = out_ref.shape[3], out_ref.shape[2]
    scale = jnp.sum(peak_ref[0], axis=0) * (1.0 / TOP)
    scale = jnp.concatenate([scale[0:1], scale[1:2]], axis=1)
    for r in range(8):
        lanes = in_ref[0, pl.ds(r, channels, stride=8), :].T * scale
        for m in range(128 // bins):
            out_ref[0, m * 8 + r] = lanes[m * bins : (m + 1) * bins]


def on_device(nx, ng, voltages, weights):
    v = voltages[0]
    streams, parts, channels, samples = v.shape
    rows, chans, half = streams * parts, channels // ng, samples // nx
    per = chans // CHUNKS
    group = ng // 2
    antennas = group * streams
    beams = weights.shape[3]
    own = beams // ng
    packs = own // 8
    bins = half // 8

    turned_weights = jnp.swapaxes(weights, 3, 4)
    hbm = pl.BlockSpec(memory_space=pltpu.HBM)
    anywhere = pl.BlockSpec(memory_space=pl.ANY)
    packed, peaks = pl.pallas_call(
        functools.partial(kernel, nx, ng),
        out_shape=(
            jax.ShapeDtypeStruct((2, ng, CHUNKS, per * 8, 128), jnp.float32),
            jax.ShapeDtypeStruct((2, group, 2, 128), jnp.float32),
        ),
        in_specs=[hbm, hbm],
        out_specs=(anywhere, anywhere),
        scratch_shapes=[
            pltpu.VMEM((rows * chans, rows * chans), jnp.bfloat16),
            pltpu.VMEM((4 * antennas, 2 * antennas), jnp.bfloat16),
            pltpu.VMEM((packs, half, 128), jnp.bfloat16),
            pltpu.VMEM((2 * group, streams, parts, chans, samples), jnp.bfloat16),
            pltpu.VMEM((2 * CHUNKS, nx * group, per, rows, half), jnp.bfloat16),
            pltpu.VMEM((2 * CHUNKS, nx * group, per, rows, half), jnp.bfloat16),
            pltpu.VMEM(turned_weights.shape, jnp.bfloat16),
            pltpu.VMEM((ng, per, 8, 128), jnp.float32),
            pltpu.VMEM((2 * CHUNKS, ng, per * 8, 128), jnp.bfloat16),
            pltpu.VMEM((2, ng, CHUNKS, per * 8, 128), jnp.bfloat16),
            pltpu.VMEM((2, ng, CHUNKS, per * 8, 128), jnp.float32),
            pltpu.VMEM((2, 128), jnp.float32),
            pltpu.SemaphoreType.DMA((2 * group,)),
            pltpu.SemaphoreType.REGULAR,
            pltpu.SemaphoreType.DMA,
            pltpu.SemaphoreType.DMA,
            pltpu.SemaphoreType.DMA((PIECES,)),
            pltpu.SemaphoreType.DMA,
            pltpu.SemaphoreType.DMA((PIECES,)),
            pltpu.SemaphoreType.DMA((2 * CHUNKS,)),
            pltpu.SemaphoreType.DMA((2 * CHUNKS,)),
            pltpu.SemaphoreType.DMA,
            pltpu.SemaphoreType.DMA((2 * CHUNKS,)),
            pltpu.SemaphoreType.DMA,
            pltpu.SemaphoreType.DMA,
            pltpu.SemaphoreType.DMA,
        ],
        compiler_params=pltpu.CompilerParams(
            collective_id=0, has_side_effects=True, vmem_limit_bytes=VMEM
        ),
    )(v, turned_weights)

    spread = pl.pallas_call(
        spread_kernel,
        grid=(2,),
        out_shape=jax.ShapeDtypeStruct((2, own, bins, channels), jnp.float32),
        in_specs=[
            pl.BlockSpec((1, channels * 8, 128), lambda q: (q, 0, 0)),
            pl.BlockSpec((1, group, 2, 128), lambda q: (q, 0, 0, 0)),
        ],
        out_specs=pl.BlockSpec((1, own, bins, channels), lambda q: (q, 0, 0, 0)),
        compiler_params=pltpu.CompilerParams(vmem_limit_bytes=VMEM),
    )(packed.reshape(2, channels * 8, 128), peaks)
    return spread.transpose(3, 0, 1, 2)


def solution(mesh):
    nx, ng = mesh.shape["ta"], mesh.shape["gx"]

    def body(voltages, weights):
        _, streams, parts, channels, samples = voltages.shape
        rows, chans, half = streams * parts, channels // ng, samples // nx
        own = weights.shape[3] // ng
        fits = (
            nx == 2
            and rows % 16 == 0
            and chans % 16 == 0
            and half % 128 == 0
            and own % 8 == 0
            and (own // 8) * (half // 8) == 128
            and ng % 2 == 0
            and ng & (ng - 1) == 0
            and ng * chans == 256
        )
        if fits:
            return on_device(nx, ng, voltages, weights)
        return plain_on_device(voltages, weights)

    in_specs = (P("ta", "gx", None, None, None), P(None, "gx", None, None, None))
    out_specs = P(None, None, "gx", "ta")
    return jax.shard_map(
        body, mesh=mesh, in_specs=in_specs, out_specs=out_specs, check_vma=False
    )
```

```python
import functools

import jax
import jax.numpy as jnp
from jax import lax
from jax.experimental import pallas as pl
from jax.experimental.pallas import tpu as pltpu
from jax.sharding import PartitionSpec as P

MESH = pl.DeviceIdType.MESH
VMEM = 48 * 1024 * 1024
CHUNKS = 4
PIECES = 4
HOLD = 2
LEAD = 8
NEAR = 2
TOP = 2.0**15.75
FLOOR = 2.0**-90
NEXT = 1.0 + 1.3 / 256


def beam_power(voltage, weight_block):
    antennas = weight_block.shape[3]
    beam_count = weight_block.shape[2]
    powers = []
    for side_index in range(2):
        real_w = weight_block[side_index, 0]
        imag_w = weight_block[side_index, 1]
        upper_rows = jnp.stack([real_w, -imag_w], axis=-1).reshape(beam_count, 2 * antennas)
        bottom_half_rows = jnp.stack([imag_w, real_w], axis=-1).reshape(beam_count, 2 * antennas)
        matrix = jnp.concatenate([upper_rows, bottom_half_rows], 0)
        signal = voltage[side_index * antennas : (side_index + 1) * antennas].reshape(
            2 * antennas, -1
        )
        beam_voltage_field = jnp.dot(matrix, signal, preferred_element_type=jnp.float32)
        power = (
            beam_voltage_field[:beam_count] * beam_voltage_field[:beam_count]
            + beam_voltage_field[beam_count:] * beam_voltage_field[beam_count:]
        )
        powers.append(power.reshape(beam_count, -1, 8).sum(-1))
    return jnp.stack(powers, 0)


def channel_powers(turned, weights):

    def one_channel(column):
        voltage = lax.dynamic_index_in_dim(turned, column, 2, keepdims=False)
        weight_block = lax.dynamic_index_in_dim(weights, column, 1, keepdims=False)
        return beam_power(voltage, weight_block)

    return lax.map(one_channel, jnp.arange(turned.shape[2], dtype=jnp.int32))


def plain_on_device(voltages, weights):
    turned = lax.all_to_all(voltages, "gx", split_axis=3, concat_axis=1, tiled=True)
    partial_power_value = channel_powers(turned[0], weights)
    relaid = lax.all_to_all(partial_power_value, "gx", split_axis=2, concat_axis=0, tiled=True)
    return lax.psum_scatter(relaid, "ta", scatter_dimension=3, tiled=True)


def kernel(
    nx, ng, v_hbm, w_hbm, out_ref, peak_ref,
    turn_ref, mix_ref, gather_ref, vbuf, sbuf, vrecv, w_ref, work, pbuf, codes, plain, peaks,
    v_sem, cross, w_sem, wsend, wz, relay_sem, wx, vsend, vget, psend, pget, msend, mget, out_sem,
):
    x = lax.axis_index("ta")
    g = lax.axis_index("gx")
    rows = v_hbm.shape[0] * v_hbm.shape[1]
    chans = v_hbm.shape[2] // ng
    half = v_hbm.shape[3] // nx
    per = chans // CHUNKS
    group = ng // 2
    antennas2 = group * rows
    beams = w_ref.shape[4]
    side = g // group
    u = lax.rem(g, group)
    partner = lax.rem(g + group, ng)
    steps = 2 * CHUNKS
    dests = nx * group
    mine = x * group + u
    piece = chans // nx // PIECES

    barrier = pltpu.get_barrier_semaphore()

    def greet(i, _):
        d = mine ^ i
        pl.semaphore_signal(
            barrier,
            inc=1,
            device_id=(d // group, side * group + lax.rem(d, group)),
            device_id_type=MESH,
        )
        return 0

    lax.fori_loop(1, dests, greet, 0)
    pl.semaphore_signal(barrier, inc=1, device_id=(x, partner), device_id_type=MESH)

    w_copy = pltpu.make_async_copy(w_hbm.at[side], w_ref.at[0], w_sem)

    def fetch(block):
        return pltpu.make_async_copy(
            v_hbm.at[:, :, pl.ds(pl.multiple_of(block * chans, chans), chans), :],
            vbuf.at[block],
            v_sem.at[block],
        )

    def fetch_side(which):
        def start(i, _):
            fetch(which * group + (u ^ (group - 1 - i))).start()
            return 0

        lax.fori_loop(0, group, start, 0)

    fetch_side(side)
    fetch_side(1 - side)
    w_copy.start()

    def grid_of(shape):
        return [lax.broadcasted_iota(jnp.int32, shape, axis) for axis in (0, 1)]

    i, j = grid_of(turn_ref.shape)
    hit = (j % chans == i // rows) & (j // chans == i % rows)
    turn_ref[...] = hit.astype(jnp.float32).astype(jnp.bfloat16)

    def turn_block(which, b):
        base = lax.rem(which + side, 2) * CHUNKS
        fetch(which * group + b).wait()
        block = vbuf[which * group + b].reshape(rows * chans, nx * half)
        turned = jnp.dot(turn_ref[...], block, preferred_element_type=jnp.float32)
        turned = turned.astype(jnp.bfloat16).reshape(CHUNKS, per, rows, nx * half)
        for k in range(nx):
            sbuf[pl.ds(base, CHUNKS), k * group + b] = turned[
                :, :, :, k * half : (k + 1) * half
            ]

    def send_voltage(k, d):
        first = k // CHUNKS * CHUNKS
        skew = k // CHUNKS * (CHUNKS // nx)
        return pltpu.make_async_remote_copy(
            src_ref=sbuf.at[first + lax.rem(k - first + d // group * skew, CHUNKS), d],
            dst_ref=vrecv.at[k, mine],
            send_sem=vsend.at[k],
            recv_sem=vget.at[k],
            device_id=(d // group, side * group + lax.rem(d, group)),
            device_id_type=MESH,
        )

    def keep_voltages(k):
        first = k // CHUNKS * CHUNKS
        skew = k // CHUNKS * (CHUNKS // nx)
        own = sbuf.at[first + lax.rem(k - first + x * skew, CHUNKS), mine]
        pltpu.make_async_copy(own, vrecv.at[k, mine], vget.at[k]).start()

    def send_voltages(k):
        keep_voltages(k)

        def send(i, _):
            send_voltage(k, mine ^ (dests - i)).start()
            return 0

        lax.fori_loop(1, dests, send, 0)

    def send_weights(i):
        span = pl.ds((x * PIECES + i) * piece, piece)
        pltpu.make_async_remote_copy(
            src_ref=w_hbm.at[1 - side, span],
            dst_ref=w_ref.at[1, span],
            send_sem=wsend,
            recv_sem=wz.at[i],
            device_id=(x, partner),
            device_id_type=MESH,
        ).start()

    def relay_weights(i):
        block = w_ref.at[1, pl.ds((x * PIECES + i) * piece, piece)]
        pltpu.make_async_copy(block, block, wz.at[i]).wait()
        pltpu.make_async_remote_copy(
            src_ref=block,
            dst_ref=block,
            send_sem=relay_sem,
            recv_sem=wx.at[i],
            device_id=(1 - x, g),
            device_id_type=MESH,
        ).start()

    pl.semaphore_wait(barrier, dests)
    pl.semaphore_signal(cross, inc=1, device_id=(x, partner), device_id_type=MESH)

    def turn_and_send(i, _):
        @pl.when(i > 0)
        def _():
            b = u ^ (group - i)
            send_voltage(0, (1 - x) * group + b).start()
            send_voltage(0, x * group + b).start()

        turn_block(side, u ^ (group - 1 - i))
        return 0

    lax.fori_loop(0, group, turn_and_send, 0)
    send_weights(0)
    send_voltage(0, (1 - x) * group + u).start()
    keep_voltages(0)
    for k in range(1, CHUNKS):
        send_voltages(k)
        send_weights(k)

    def turn(i, _):
        turn_block(1 - side, i)
        return 0

    lax.fori_loop(0, group, turn, 0)
    for k in range(CHUNKS, LEAD):
        send_voltages(k)
    antennas = antennas2 // 2
    i, j = grid_of(mix_ref.shape)
    block = i // antennas
    wants = 2 * (i % antennas) + ((block == 1) | (block == 2)).astype(jnp.int32)
    sign = jnp.where(block == 1, -1.0, 1.0)
    mix_ref[...] = jnp.where(j == wants, sign, 0.0).astype(jnp.bfloat16)
    sample, lane = grid_of(gather_ref.shape[1:])
    for m in range(gather_ref.shape[0]):
        hit = lane == m * (half // 8) + sample // 8
        gather_ref[m] = hit.astype(jnp.float32).astype(jnp.bfloat16)
    w_copy.wait()

    def power_slot(k):
        which = k // CHUNKS
        part_of = lax.rem(k + which * x * (CHUNKS // nx), CHUNKS)
        return codes.at[side, lax.rem(g + which * group, ng), part_of]

    def send_powers(k, d):
        pltpu.make_async_remote_copy(
            src_ref=pbuf.at[k, d],
            dst_ref=power_slot(k),
            send_sem=psend,
            recv_sem=pget.at[k],
            device_id=(x, d),
            device_id_type=MESH,
        ).start()

    def send_near(k):
        pltpu.make_async_copy(pbuf.at[k, g], power_slot(k), pget.at[k]).start()

        def send(i, _):
            send_powers(k, g ^ (group - i))
            return 0

        lax.fori_loop(1, group, send, 0)

    def step(k, _):
        pltpu.make_async_copy(vrecv.at[k], vrecv.at[k], vget.at[k]).wait()

        @pl.when(k + LEAD < steps)
        def _():
            send_voltages(k + LEAD)

        @pl.when((k >= HOLD) & (k < HOLD + PIECES))
        def _():
            relay_weights(k - HOLD)

        for i in range(PIECES):

            @pl.when(k == steps - CHUNKS // nx + i * CHUNKS // nx // PIECES)
            def _(i=i):
                other = w_ref.at[1, pl.ds(((1 - x) * PIECES + i) * piece, piece)]
                pltpu.make_async_copy(other, other, wx.at[i]).wait()

        which = k // CHUNKS
        part_of = lax.rem(k + which * x * (CHUNKS // nx), CHUNKS)

        def channel(c, peak):
            w = w_ref[which, part_of * per + c].reshape(antennas2, beams).T
            power = None
            for h in range(nx):
                v = vrecv[k, h * group : (h + 1) * group, c].reshape(antennas2, half)
                mixed = jnp.dot(mix_ref[...], v, preferred_element_type=jnp.float32)
                mixed = mixed.astype(jnp.bfloat16)
                re = jnp.dot(w, mixed[:antennas2], preferred_element_type=jnp.float32)
                im = jnp.dot(w, mixed[antennas2:], preferred_element_type=jnp.float32)
                part = re * re + im * im
                power = part if power is None else power + part
            own = beams // ng
            packs = own // 8
            power = power.reshape(ng, packs, 8, half)
            total = None
            for m in range(packs):
                p = power[:, m].reshape(ng * 8, half)
                high = p.astype(jnp.bfloat16)
                low = (p - high.astype(jnp.float32)).astype(jnp.bfloat16)
                t = jnp.dot(high, gather_ref[m], preferred_element_type=jnp.float32)
                t += jnp.dot(low, gather_ref[m], preferred_element_type=jnp.float32)
                total = t if total is None else total + t
            total = total.reshape(ng, 8, 128)
            work[:, pl.ds(c, 1)] = total[:, None]
            return jnp.maximum(peak, jnp.max(total, axis=0))

        peak = lax.fori_loop(0, per, channel, jnp.zeros((8, 128), jnp.float32))
        peak = jnp.maximum(jnp.max(peak, keepdims=True), FLOOR)
        code = work[...].reshape(ng, per * 8, 128) * (TOP / peak)[None]
        code = code * code
        code = code * code
        code = code * code
        near = code.astype(jnp.bfloat16).astype(jnp.float32)
        pbuf[k] = jnp.where(code < near, -near, near).astype(jnp.bfloat16)
        row = lax.broadcasted_iota(jnp.int32, peaks.shape, 0)
        lane = lax.broadcasted_iota(jnp.int32, peaks.shape, 1)
        own_row = lax.rem(side + which, 2)
        first = u * chans + part_of * per
        held = (row == own_row) & (lane >= first) & (lane < first + per)
        peaks[...] = jnp.where(held, peak, peaks[...])

        @pl.when(k == 0)
        def _():
            pl.semaphore_wait(cross, 1)

        def send(i, _):
            send_powers(k, (1 - side) * group + i)
            return 0

        lax.fori_loop(0, group, send, 0)

        @pl.when(side == 0)
        def _():
            send_near(k)

        @pl.when((side == 1) & (k >= NEAR))
        def _():
            send_near(k - NEAR)

        return 0

    peaks[...] = jnp.zeros_like(peaks)
    lax.fori_loop(0, steps, step, 0)

    pltpu.make_async_copy(peaks, peak_ref.at[side, u], mget).start()

    def send_peaks(i, _):
        pltpu.make_async_remote_copy(
            src_ref=peaks,
            dst_ref=peak_ref.at[side, u],
            send_sem=msend,
            recv_sem=mget,
            device_id=(x, lax.rem(g + i, ng)),
            device_id_type=MESH,
        ).start()
        return 0

    lax.fori_loop(1, ng, send_peaks, 0)

    @pl.when(side == 1)
    def _():
        def late(k, _):
            send_near(k)
            return 0

        lax.fori_loop(steps - NEAR, steps, late, 0)

    def decode(k, _):
        pltpu.make_async_copy(pbuf.at[k], pbuf.at[k], pget.at[k]).wait()
        which = k // CHUNKS
        part_of = lax.rem(k + which * x * (CHUNKS // nx), CHUNKS)
        for other in range(2):
            span = pl.ds((other + which) % 2 * group, group)
            code = codes[other, span, part_of].astype(jnp.float32)
            near = jnp.abs(code)
            gap = (near * NEXT).astype(jnp.bfloat16).astype(jnp.float32) - near
            near = near + jnp.where(code < 0, -0.25, 0.25) * gap
            plain[other, span, part_of] = jnp.exp(jnp.log(near) * 0.125)
            pltpu.make_async_copy(
                plain.at[other, span, part_of],
                out_ref.at[other, span, part_of],
                out_sem,
            ).start()
        return 0

    lax.fori_loop(0, steps, decode, 0)
    pltpu.make_async_copy(peak_ref, peak_ref, mget).wait()
    pltpu.make_async_copy(out_ref, out_ref, out_sem).wait()
    for k in range(steps):
        sent = sbuf.at[k, pl.ds(0, dests - 1)]
        pltpu.make_async_copy(sent, sent, vsend.at[k]).wait()
    sent = pbuf.at[:, pl.ds(0, ng - 1)]
    pltpu.make_async_copy(sent, sent, psend).wait()
    sent = peak_ref.at[:, pl.ds(0, group - 1)]
    pltpu.make_async_copy(sent, sent, msend).wait()
    sent = peak_ref.at[0, pl.ds(0, 1)]
    pltpu.make_async_copy(sent, sent, msend).wait()
    sent = w_ref.at[1, pl.ds(0, PIECES * piece)]
    pltpu.make_async_copy(sent, sent, wsend).wait()
    pltpu.make_async_copy(sent, sent, relay_sem).wait()


def spread_kernel(in_ref, peak_ref, out_ref):
    channels, bins = out_ref.shape[3], out_ref.shape[2]
    scale = jnp.sum(peak_ref[0], axis=0) * (1.0 / TOP)
    scale = jnp.concatenate([scale[0:1], scale[1:2]], axis=1)
    for r in range(8):
        lanes = in_ref[0, pl.ds(r, channels, stride=8), :].T * scale
        for m in range(128 // bins):
            out_ref[0, m * 8 + r] = lanes[m * bins : (m + 1) * bins]


def on_device(nx, ng, voltages, weights):
    v = voltages[0]
    streams, parts, channels, samples = v.shape
    rows, chans, half = streams * parts, channels // ng, samples // nx
    per = chans // CHUNKS
    group = ng // 2
    antennas = group * streams
    beams = weights.shape[3]
    own = beams // ng
    packs = own // 8
    bins = half // 8

    turned_weights = jnp.swapaxes(weights, 3, 4)
    hbm = pl.BlockSpec(memory_space=pltpu.HBM)
    anywhere = pl.BlockSpec(memory_space=pl.ANY)
    packed, peaks = pl.pallas_call(
        functools.partial(kernel, nx, ng),
        out_shape=(
            jax.ShapeDtypeStruct((2, ng, CHUNKS, per * 8, 128), jnp.float32),
            jax.ShapeDtypeStruct((2, group, 2, 128), jnp.float32),
        ),
        in_specs=[hbm, hbm],
        out_specs=(anywhere, anywhere),
        scratch_shapes=[
            pltpu.VMEM((rows * chans, rows * chans), jnp.bfloat16),
            pltpu.VMEM((4 * antennas, 2 * antennas), jnp.bfloat16),
            pltpu.VMEM((packs, half, 128), jnp.bfloat16),
            pltpu.VMEM((2 * group, streams, parts, chans, samples), jnp.bfloat16),
            pltpu.VMEM((2 * CHUNKS, nx * group, per, rows, half), jnp.bfloat16),
            pltpu.VMEM((2 * CHUNKS, nx * group, per, rows, half), jnp.bfloat16),
            pltpu.VMEM(turned_weights.shape, jnp.bfloat16),
            pltpu.VMEM((ng, per, 8, 128), jnp.float32),
            pltpu.VMEM((2 * CHUNKS, ng, per * 8, 128), jnp.bfloat16),
            pltpu.VMEM((2, ng, CHUNKS, per * 8, 128), jnp.bfloat16),
            pltpu.VMEM((2, ng, CHUNKS, per * 8, 128), jnp.float32),
            pltpu.VMEM((2, 128), jnp.float32),
            pltpu.SemaphoreType.DMA((2 * group,)),
            pltpu.SemaphoreType.REGULAR,
            pltpu.SemaphoreType.DMA,
            pltpu.SemaphoreType.DMA,
            pltpu.SemaphoreType.DMA((PIECES,)),
            pltpu.SemaphoreType.DMA,
            pltpu.SemaphoreType.DMA((PIECES,)),
            pltpu.SemaphoreType.DMA((2 * CHUNKS,)),
            pltpu.SemaphoreType.DMA((2 * CHUNKS,)),
            pltpu.SemaphoreType.DMA,
            pltpu.SemaphoreType.DMA((2 * CHUNKS,)),
            pltpu.SemaphoreType.DMA,
            pltpu.SemaphoreType.DMA,
            pltpu.SemaphoreType.DMA,
        ],
        compiler_params=pltpu.CompilerParams(
            collective_id=0, has_side_effects=True, vmem_limit_bytes=VMEM
        ),
    )(v, turned_weights)

    spread = pl.pallas_call(
        spread_kernel,
        grid=(2,),
        out_shape=jax.ShapeDtypeStruct((2, own, bins, channels), jnp.float32),
        in_specs=[
            pl.BlockSpec((1, channels * 8, 128), lambda q: (q, 0, 0)),
            pl.BlockSpec((1, group, 2, 128), lambda q: (q, 0, 0, 0)),
        ],
        out_specs=pl.BlockSpec((1, own, bins, channels), lambda q: (q, 0, 0, 0)),
        compiler_params=pltpu.CompilerParams(vmem_limit_bytes=VMEM),
    )(packed.reshape(2, channels * 8, 128), peaks)
    return spread.transpose(3, 0, 1, 2)


def solution(mesh):
    nx, ng = mesh.shape["ta"], mesh.shape["gx"]

    def body(voltages, weights):
        _, streams, parts, channels, samples = voltages.shape
        rows, chans, half = streams * parts, channels // ng, samples // nx
        own = weights.shape[3] // ng
        fits = (
            nx == 2
            and rows % 16 == 0
            and chans % 16 == 0
            and half % 128 == 0
            and own % 8 == 0
            and (own // 8) * (half // 8) == 128
            and ng % 2 == 0
            and ng & (ng - 1) == 0
            and ng * chans == 256
        )
        if fits:
            return on_device(nx, ng, voltages, weights)
        return plain_on_device(voltages, weights)

    in_specs = (P("ta", "gx", None, None, None), P(None, "gx", None, None, None))
    out_specs = P(None, None, "gx", "ta")
    return jax.shard_map(
        body, mesh=mesh, in_specs=in_specs, out_specs=out_specs, check_vma=False
    )
```

```python
import functools

import jax
import jax.numpy as jnp
from jax import lax
from jax.experimental import pallas as pl
from jax.experimental.pallas import tpu as pltpu
from jax.sharding import PartitionSpec as P

MESH = pl.DeviceIdType.MESH
VMEM = 48 * 1024 * 1024
CHUNKS = 4
PIECES = 4
HOLD = 2
LEAD = 8
NEAR = 3
TOP = 2.0**15.75
FLOOR = 2.0**-90
NEXT = 1.0 + 1.3 / 256


def beam_power(voltage, weight_block):
    antennas = weight_block.shape[3]
    beam_count = weight_block.shape[2]
    powers = []
    for side_index in range(2):
        real_w = weight_block[side_index, 0]
        imag_w = weight_block[side_index, 1]
        upper_rows = jnp.stack([real_w, -imag_w], axis=-1).reshape(beam_count, 2 * antennas)
        bottom_half_rows = jnp.stack([imag_w, real_w], axis=-1).reshape(beam_count, 2 * antennas)
        matrix = jnp.concatenate([upper_rows, bottom_half_rows], 0)
        signal = voltage[side_index * antennas : (side_index + 1) * antennas].reshape(
            2 * antennas, -1
        )
        beam_voltage_field = jnp.dot(matrix, signal, preferred_element_type=jnp.float32)
        power = (
            beam_voltage_field[:beam_count] * beam_voltage_field[:beam_count]
            + beam_voltage_field[beam_count:] * beam_voltage_field[beam_count:]
        )
        powers.append(power.reshape(beam_count, -1, 8).sum(-1))
    return jnp.stack(powers, 0)


def channel_powers(turned, weights):

    def one_channel(column):
        voltage = lax.dynamic_index_in_dim(turned, column, 2, keepdims=False)
        weight_block = lax.dynamic_index_in_dim(weights, column, 1, keepdims=False)
        return beam_power(voltage, weight_block)

    return lax.map(one_channel, jnp.arange(turned.shape[2], dtype=jnp.int32))


def plain_on_device(voltages, weights):
    turned = lax.all_to_all(voltages, "gx", split_axis=3, concat_axis=1, tiled=True)
    partial_power_value = channel_powers(turned[0], weights)
    relaid = lax.all_to_all(partial_power_value, "gx", split_axis=2, concat_axis=0, tiled=True)
    return lax.psum_scatter(relaid, "ta", scatter_dimension=3, tiled=True)


def kernel(
    nx, ng, v_hbm, w_hbm, out_ref, peak_ref,
    turn_ref, mix_ref, gather_ref, vbuf, sbuf, vrecv, w_ref, work, pbuf, codes, plain, peaks,
    v_sem, cross, w_sem, wsend, wz, relay_sem, wx, vsend, vget, psend, pget, msend, mget, out_sem,
):
    x = lax.axis_index("ta")
    g = lax.axis_index("gx")
    rows = v_hbm.shape[0] * v_hbm.shape[1]
    chans = v_hbm.shape[2] // ng
    half = v_hbm.shape[3] // nx
    per = chans // CHUNKS
    group = ng // 2
    antennas2 = group * rows
    beams = w_ref.shape[4]
    side = g // group
    u = lax.rem(g, group)
    partner = lax.rem(g + group, ng)
    last = (side == 1) & (u >= group // 2)
    steps = 2 * CHUNKS
    dests = nx * group
    mine = x * group + u
    piece = chans // nx // PIECES

    barrier = pltpu.get_barrier_semaphore()

    def greet(i, _):
        d = mine ^ i
        pl.semaphore_signal(
            barrier,
            inc=1,
            device_id=(d // group, side * group + lax.rem(d, group)),
            device_id_type=MESH,
        )
        return 0

    lax.fori_loop(1, dests, greet, 0)
    pl.semaphore_signal(barrier, inc=1, device_id=(x, partner), device_id_type=MESH)

    w_copy = pltpu.make_async_copy(w_hbm.at[side], w_ref.at[0], w_sem)

    def fetch(block):
        return pltpu.make_async_copy(
            v_hbm.at[:, :, pl.ds(pl.multiple_of(block * chans, chans), chans), :],
            vbuf.at[block],
            v_sem.at[block],
        )

    def fetch_side(which):
        def start(i, _):
            fetch(which * group + (u ^ (group - 1 - i))).start()
            return 0

        lax.fori_loop(0, group, start, 0)

    fetch_side(side)
    fetch_side(1 - side)
    w_copy.start()

    def grid_of(shape):
        return [lax.broadcasted_iota(jnp.int32, shape, axis) for axis in (0, 1)]

    i, j = grid_of(turn_ref.shape)
    hit = (j % chans == i // rows) & (j // chans == i % rows)
    turn_ref[...] = hit.astype(jnp.float32).astype(jnp.bfloat16)

    def turn_block(which, b):
        base = lax.rem(which + side, 2) * CHUNKS
        fetch(which * group + b).wait()
        block = vbuf[which * group + b].reshape(rows * chans, nx * half)
        turned = jnp.dot(turn_ref[...], block, preferred_element_type=jnp.float32)
        turned = turned.astype(jnp.bfloat16).reshape(CHUNKS, per, rows, nx * half)
        for k in range(nx):
            sbuf[pl.ds(base, CHUNKS), k * group + b] = turned[
                :, :, :, k * half : (k + 1) * half
            ]

    def send_voltage(k, d):
        first = k // CHUNKS * CHUNKS
        skew = k // CHUNKS * (CHUNKS // nx)
        return pltpu.make_async_remote_copy(
            src_ref=sbuf.at[first + lax.rem(k - first + d // group * skew, CHUNKS), d],
            dst_ref=vrecv.at[k, mine],
            send_sem=vsend.at[k],
            recv_sem=vget.at[k],
            device_id=(d // group, side * group + lax.rem(d, group)),
            device_id_type=MESH,
        )

    def keep_voltages(k):
        first = k // CHUNKS * CHUNKS
        skew = k // CHUNKS * (CHUNKS // nx)
        own = sbuf.at[first + lax.rem(k - first + x * skew, CHUNKS), mine]
        pltpu.make_async_copy(own, vrecv.at[k, mine], vget.at[k]).start()

    def send_voltages(k):
        keep_voltages(k)

        def send(i, _):
            send_voltage(k, mine ^ (dests - i)).start()
            return 0

        lax.fori_loop(1, dests, send, 0)

    def send_weights(i):
        span = pl.ds((x * PIECES + i) * piece, piece)
        pltpu.make_async_remote_copy(
            src_ref=w_hbm.at[1 - side, span],
            dst_ref=w_ref.at[1, span],
            send_sem=wsend,
            recv_sem=wz.at[i],
            device_id=(x, partner),
            device_id_type=MESH,
        ).start()

    def relay_weights(i):
        block = w_ref.at[1, pl.ds((x * PIECES + i) * piece, piece)]
        pltpu.make_async_copy(block, block, wz.at[i]).wait()
        pltpu.make_async_remote_copy(
            src_ref=block,
            dst_ref=block,
            send_sem=relay_sem,
            recv_sem=wx.at[i],
            device_id=(1 - x, g),
            device_id_type=MESH,
        ).start()

    pl.semaphore_wait(barrier, dests)
    pl.semaphore_signal(cross, inc=1, device_id=(x, partner), device_id_type=MESH)

    send_weights(0)

    def turn_and_send(i, _):
        @pl.when(i > 0)
        def _():
            b = u ^ (group - i)
            send_voltage(0, (1 - x) * group + b).start()
            send_voltage(0, x * group + b).start()

        turn_block(side, u ^ (group - 1 - i))
        return 0

    lax.fori_loop(0, group, turn_and_send, 0)
    send_voltage(0, (1 - x) * group + u).start()
    keep_voltages(0)
    for k in range(1, CHUNKS):
        send_voltages(k)
        send_weights(k)

    def turn(i, _):
        turn_block(1 - side, i)
        return 0

    lax.fori_loop(0, group, turn, 0)
    for k in range(CHUNKS, LEAD):
        send_voltages(k)
    antennas = antennas2 // 2
    i, j = grid_of(mix_ref.shape)
    block = i // antennas
    wants = 2 * (i % antennas) + ((block == 1) | (block == 2)).astype(jnp.int32)
    sign = jnp.where(block == 1, -1.0, 1.0)
    mix_ref[...] = jnp.where(j == wants, sign, 0.0).astype(jnp.bfloat16)
    sample, lane = grid_of(gather_ref.shape[1:])
    for m in range(gather_ref.shape[0]):
        hit = lane == m * (half // 8) + sample // 8
        gather_ref[m] = hit.astype(jnp.float32).astype(jnp.bfloat16)
    w_copy.wait()

    def power_slot(k):
        which = k // CHUNKS
        part_of = lax.rem(k + which * x * (CHUNKS // nx), CHUNKS)
        return codes.at[side, lax.rem(g + which * group, ng), part_of]

    def send_powers(k, d):
        pltpu.make_async_remote_copy(
            src_ref=pbuf.at[k, d],
            dst_ref=power_slot(k),
            send_sem=psend,
            recv_sem=pget.at[k],
            device_id=(x, d),
            device_id_type=MESH,
        ).start()

    def send_near(k):
        pltpu.make_async_copy(pbuf.at[k, g], power_slot(k), pget.at[k]).start()

        def send(i, _):
            send_powers(k, g ^ (group - i))
            return 0

        lax.fori_loop(1, group, send, 0)

    def step(k, _):
        pltpu.make_async_copy(vrecv.at[k], vrecv.at[k], vget.at[k]).wait()

        @pl.when(k + LEAD < steps)
        def _():
            send_voltages(k + LEAD)

        @pl.when((k >= HOLD) & (k < HOLD + PIECES))
        def _():
            relay_weights(k - HOLD)

        for i in range(PIECES):

            @pl.when(k == steps - CHUNKS // nx + i * CHUNKS // nx // PIECES)
            def _(i=i):
                other = w_ref.at[1, pl.ds(((1 - x) * PIECES + i) * piece, piece)]
                pltpu.make_async_copy(other, other, wx.at[i]).wait()

        which = k // CHUNKS
        part_of = lax.rem(k + which * x * (CHUNKS // nx), CHUNKS)

        def channel(c, peak):
            w = w_ref[which, part_of * per + c].reshape(antennas2, beams).T
            power = None
            for h in range(nx):
                v = vrecv[k, h * group : (h + 1) * group, c].reshape(antennas2, half)
                mixed = jnp.dot(mix_ref[...], v, preferred_element_type=jnp.float32)
                mixed = mixed.astype(jnp.bfloat16)
                re = jnp.dot(w, mixed[:antennas2], preferred_element_type=jnp.float32)
                im = jnp.dot(w, mixed[antennas2:], preferred_element_type=jnp.float32)
                part = re * re + im * im
                power = part if power is None else power + part
            own = beams // ng
            packs = own // 8
            power = power.reshape(ng, packs, 8, half)
            total = None
            for m in range(packs):
                p = power[:, m].reshape(ng * 8, half)
                high = p.astype(jnp.bfloat16)
                low = (p - high.astype(jnp.float32)).astype(jnp.bfloat16)
                t = jnp.dot(high, gather_ref[m], preferred_element_type=jnp.float32)
                t += jnp.dot(low, gather_ref[m], preferred_element_type=jnp.float32)
                total = t if total is None else total + t
            total = total.reshape(ng, 8, 128)
            work[:, pl.ds(c, 1)] = total[:, None]
            return jnp.maximum(peak, jnp.max(total, axis=0))

        peak = lax.fori_loop(0, per, channel, jnp.zeros((8, 128), jnp.float32))
        peak = jnp.maximum(jnp.max(peak, keepdims=True), FLOOR)
        code = work[...].reshape(ng, per * 8, 128) * (TOP / peak)[None]
        code = code * code
        code = code * code
        code = code * code
        near = code.astype(jnp.bfloat16).astype(jnp.float32)
        pbuf[k] = jnp.where(code < near, -near, near).astype(jnp.bfloat16)
        row = lax.broadcasted_iota(jnp.int32, peaks.shape, 0)
        lane = lax.broadcasted_iota(jnp.int32, peaks.shape, 1)
        own_row = lax.rem(side + which, 2)
        first = u * chans + part_of * per
        held = (row == own_row) & (lane >= first) & (lane < first + per)
        peaks[...] = jnp.where(held, peak, peaks[...])

        @pl.when(k == 0)
        def _():
            pl.semaphore_wait(cross, 1)

        def send(i, _):
            send_powers(k, (1 - side) * group + i)
            return 0

        @pl.when(side == 0)
        def _():
            send_near(k)

        lax.fori_loop(0, group, send, 0)

        @pl.when(~last & (side == 1))
        def _():
            send_near(k)

        @pl.when(last & (k >= NEAR))
        def _():
            send_near(k - NEAR)

        return 0

    peaks[...] = jnp.zeros_like(peaks)
    lax.fori_loop(0, steps, step, 0)

    pltpu.make_async_copy(peaks, peak_ref.at[side, u], mget).start()

    def send_peaks(i, _):
        pltpu.make_async_remote_copy(
            src_ref=peaks,
            dst_ref=peak_ref.at[side, u],
            send_sem=msend,
            recv_sem=mget,
            device_id=(x, lax.rem(g + i, ng)),
            device_id_type=MESH,
        ).start()
        return 0

    lax.fori_loop(1, ng, send_peaks, 0)

    @pl.when(last)
    def _():
        def late(k, _):
            send_near(k)
            return 0

        lax.fori_loop(steps - NEAR, steps, late, 0)

    def decode(k, _):
        pltpu.make_async_copy(pbuf.at[k], pbuf.at[k], pget.at[k]).wait()
        which = k // CHUNKS
        part_of = lax.rem(k + which * x * (CHUNKS // nx), CHUNKS)
        for other in range(2):
            span = pl.ds((other + which) % 2 * group, group)
            code = codes[other, span, part_of].astype(jnp.float32)
            near = jnp.abs(code)
            gap = (near * NEXT).astype(jnp.bfloat16).astype(jnp.float32) - near
            near = near + jnp.where(code < 0, -0.25, 0.25) * gap
            plain[other, span, part_of] = jnp.exp(jnp.log(near) * 0.125)
            pltpu.make_async_copy(
                plain.at[other, span, part_of],
                out_ref.at[other, span, part_of],
                out_sem,
            ).start()
        return 0

    lax.fori_loop(0, steps, decode, 0)
    pltpu.make_async_copy(peak_ref, peak_ref, mget).wait()
    pltpu.make_async_copy(out_ref, out_ref, out_sem).wait()
    for k in range(steps):
        sent = sbuf.at[k, pl.ds(0, dests - 1)]
        pltpu.make_async_copy(sent, sent, vsend.at[k]).wait()
    sent = pbuf.at[:, pl.ds(0, ng - 1)]
    pltpu.make_async_copy(sent, sent, psend).wait()
    sent = peak_ref.at[:, pl.ds(0, group - 1)]
    pltpu.make_async_copy(sent, sent, msend).wait()
    sent = peak_ref.at[0, pl.ds(0, 1)]
    pltpu.make_async_copy(sent, sent, msend).wait()
    sent = w_ref.at[1, pl.ds(0, PIECES * piece)]
    pltpu.make_async_copy(sent, sent, wsend).wait()
    pltpu.make_async_copy(sent, sent, relay_sem).wait()


def spread_kernel(in_ref, peak_ref, out_ref, block, sem):
    channels, bins = out_ref.shape[3], out_ref.shape[2]
    packs = 128 // bins

    def copies(q, r):
        for m in range(packs):
            yield pltpu.make_async_copy(block.at[q, m * 8 + r], out_ref.at[q, m * 8 + r], sem)

    before = None
    for q in range(2):
        scale = jnp.sum(peak_ref[q], axis=0) * (1.0 / TOP)
        scale = jnp.concatenate([scale[0:1], scale[1:2]], axis=1)
        for r in range(8):
            lanes = in_ref[q, pl.ds(r, channels, stride=8), :].T * scale
            for m in range(packs):
                block[q, m * 8 + r] = lanes[m * bins : (m + 1) * bins]
            if before is not None:
                for copy in copies(*before):
                    copy.start()
            before = (q, r)
    for copy in copies(*before):
        copy.start()
    pltpu.make_async_copy(block, out_ref, sem).wait()


def on_device(nx, ng, voltages, weights):
    v = voltages[0]
    streams, parts, channels, samples = v.shape
    rows, chans, half = streams * parts, channels // ng, samples // nx
    per = chans // CHUNKS
    group = ng // 2
    antennas = group * streams
    beams = weights.shape[3]
    own = beams // ng
    packs = own // 8
    bins = half // 8

    turned_weights = jnp.swapaxes(weights, 3, 4)
    hbm = pl.BlockSpec(memory_space=pltpu.HBM)
    anywhere = pl.BlockSpec(memory_space=pl.ANY)
    packed, peaks = pl.pallas_call(
        functools.partial(kernel, nx, ng),
        out_shape=(
            jax.ShapeDtypeStruct((2, ng, CHUNKS, per * 8, 128), jnp.float32),
            jax.ShapeDtypeStruct((2, group, 2, 128), jnp.float32),
        ),
        in_specs=[hbm, hbm],
        out_specs=(anywhere, anywhere),
        scratch_shapes=[
            pltpu.VMEM((rows * chans, rows * chans), jnp.bfloat16),
            pltpu.VMEM((4 * antennas, 2 * antennas), jnp.bfloat16),
            pltpu.VMEM((packs, half, 128), jnp.bfloat16),
            pltpu.VMEM((2 * group, streams, parts, chans, samples), jnp.bfloat16),
            pltpu.VMEM((2 * CHUNKS, nx * group, per, rows, half), jnp.bfloat16),
            pltpu.VMEM((2 * CHUNKS, nx * group, per, rows, half), jnp.bfloat16),
            pltpu.VMEM(turned_weights.shape, jnp.bfloat16),
            pltpu.VMEM((ng, per, 8, 128), jnp.float32),
            pltpu.VMEM((2 * CHUNKS, ng, per * 8, 128), jnp.bfloat16),
            pltpu.VMEM((2, ng, CHUNKS, per * 8, 128), jnp.bfloat16),
            pltpu.VMEM((2, ng, CHUNKS, per * 8, 128), jnp.float32),
            pltpu.VMEM((2, 128), jnp.float32),
            pltpu.SemaphoreType.DMA((2 * group,)),
            pltpu.SemaphoreType.REGULAR,
            pltpu.SemaphoreType.DMA,
            pltpu.SemaphoreType.DMA,
            pltpu.SemaphoreType.DMA((PIECES,)),
            pltpu.SemaphoreType.DMA,
            pltpu.SemaphoreType.DMA((PIECES,)),
            pltpu.SemaphoreType.DMA((2 * CHUNKS,)),
            pltpu.SemaphoreType.DMA((2 * CHUNKS,)),
            pltpu.SemaphoreType.DMA,
            pltpu.SemaphoreType.DMA((2 * CHUNKS,)),
            pltpu.SemaphoreType.DMA,
            pltpu.SemaphoreType.DMA,
            pltpu.SemaphoreType.DMA,
        ],
        compiler_params=pltpu.CompilerParams(
            collective_id=0, has_side_effects=True, vmem_limit_bytes=VMEM
        ),
    )(v, turned_weights)

    spread = pl.pallas_call(
        spread_kernel,
        out_shape=jax.ShapeDtypeStruct((2, own, bins, channels), jnp.float32),
        in_specs=[pl.BlockSpec(memory_space=pltpu.VMEM)] * 2,
        out_specs=anywhere,
        scratch_shapes=[
            pltpu.VMEM((2, own, bins, channels), jnp.float32),
            pltpu.SemaphoreType.DMA,
        ],
        compiler_params=pltpu.CompilerParams(vmem_limit_bytes=VMEM),
    )(packed.reshape(2, channels * 8, 128), peaks)
    return spread.transpose(3, 0, 1, 2)


def solution(mesh):
    nx, ng = mesh.shape["ta"], mesh.shape["gx"]

    def body(voltages, weights):
        _, streams, parts, channels, samples = voltages.shape
        rows, chans, half = streams * parts, channels // ng, samples // nx
        own = weights.shape[3] // ng
        fits = (
            nx == 2
            and rows % 16 == 0
            and chans % 16 == 0
            and half % 128 == 0
            and own % 8 == 0
            and (own // 8) * (half // 8) == 128
            and ng % 2 == 0
            and ng & (ng - 1) == 0
            and ng * chans == 256
        )
        if fits:
            return on_device(nx, ng, voltages, weights)
        return plain_on_device(voltages, weights)

    in_specs = (P("ta", "gx", None, None, None), P(None, "gx", None, None, None))
    out_specs = P(None, None, "gx", "ta")
    return jax.shard_map(
        body, mesh=mesh, in_specs=in_specs, out_specs=out_specs, check_vma=False
    )
```

```python
import functools

import jax
import jax.numpy as jnp
from jax import lax
from jax.experimental import pallas as pl
from jax.experimental.pallas import tpu as pltpu
from jax.sharding import PartitionSpec as P

MESH = pl.DeviceIdType.MESH
VMEM = 48 * 1024 * 1024
CHUNKS = 8
PIECES = 4
HOLD = 2
LEAD = 16
NEAR = 6
TOP = 2.0**15.75
FLOOR = 2.0**-90
NEXT = 1.0 + 1.3 / 256


def beam_power(voltage, weight_block):
    antennas = weight_block.shape[3]
    beam_count = weight_block.shape[2]
    powers = []
    for side_index in range(2):
        real_w = weight_block[side_index, 0]
        imag_w = weight_block[side_index, 1]
        upper_rows = jnp.stack([real_w, -imag_w], axis=-1).reshape(beam_count, 2 * antennas)
        bottom_half_rows = jnp.stack([imag_w, real_w], axis=-1).reshape(beam_count, 2 * antennas)
        matrix = jnp.concatenate([upper_rows, bottom_half_rows], 0)
        signal = voltage[side_index * antennas : (side_index + 1) * antennas].reshape(
            2 * antennas, -1
        )
        beam_voltage_field = jnp.dot(matrix, signal, preferred_element_type=jnp.float32)
        power = (
            beam_voltage_field[:beam_count] * beam_voltage_field[:beam_count]
            + beam_voltage_field[beam_count:] * beam_voltage_field[beam_count:]
        )
        powers.append(power.reshape(beam_count, -1, 8).sum(-1))
    return jnp.stack(powers, 0)


def channel_powers(turned, weights):

    def one_channel(column):
        voltage = lax.dynamic_index_in_dim(turned, column, 2, keepdims=False)
        weight_block = lax.dynamic_index_in_dim(weights, column, 1, keepdims=False)
        return beam_power(voltage, weight_block)

    return lax.map(one_channel, jnp.arange(turned.shape[2], dtype=jnp.int32))


def plain_on_device(voltages, weights):
    turned = lax.all_to_all(voltages, "gx", split_axis=3, concat_axis=1, tiled=True)
    partial_power_value = channel_powers(turned[0], weights)
    relaid = lax.all_to_all(partial_power_value, "gx", split_axis=2, concat_axis=0, tiled=True)
    return lax.psum_scatter(relaid, "ta", scatter_dimension=3, tiled=True)


def kernel(
    nx, ng, v_hbm, w_hbm, out_ref, peak_ref,
    turn_ref, mix_ref, gather_ref, vbuf, sbuf, vrecv, w_ref, work, pbuf, codes, plain, peaks,
    v_sem, cross, w_sem, wsend, wz, relay_sem, wx, vsend, vget, psend, pget, msend, mget, out_sem,
):
    x = lax.axis_index("ta")
    g = lax.axis_index("gx")
    rows = v_hbm.shape[0] * v_hbm.shape[1]
    chans = v_hbm.shape[2] // ng
    half = v_hbm.shape[3] // nx
    per = chans // CHUNKS
    group = ng // 2
    antennas2 = group * rows
    beams = w_ref.shape[4]
    side = g // group
    u = lax.rem(g, group)
    partner = lax.rem(g + group, ng)
    last = (side == 1) & (u >= group // 2)
    steps = 2 * CHUNKS
    dests = nx * group
    mine = x * group + u
    piece = chans // nx // PIECES

    barrier = pltpu.get_barrier_semaphore()

    def greet(i, _):
        d = mine ^ i
        pl.semaphore_signal(
            barrier,
            inc=1,
            device_id=(d // group, side * group + lax.rem(d, group)),
            device_id_type=MESH,
        )
        return 0

    lax.fori_loop(1, dests, greet, 0)
    pl.semaphore_signal(barrier, inc=1, device_id=(x, partner), device_id_type=MESH)

    w_copy = pltpu.make_async_copy(w_hbm.at[side], w_ref.at[0], w_sem)

    def fetch(block):
        return pltpu.make_async_copy(
            v_hbm.at[:, :, pl.ds(pl.multiple_of(block * chans, chans), chans), :],
            vbuf.at[block],
            v_sem.at[block],
        )

    def fetch_side(which):
        def start(i, _):
            fetch(which * group + (u ^ (group - 1 - i))).start()
            return 0

        lax.fori_loop(0, group, start, 0)

    fetch_side(side)
    fetch_side(1 - side)
    w_copy.start()

    def grid_of(shape):
        return [lax.broadcasted_iota(jnp.int32, shape, axis) for axis in (0, 1)]

    i, j = grid_of(turn_ref.shape)
    hit = (j % chans == i // rows) & (j // chans == i % rows)
    turn_ref[...] = hit.astype(jnp.float32).astype(jnp.bfloat16)

    def turn_block(which, b):
        base = lax.rem(which + side, 2) * CHUNKS
        fetch(which * group + b).wait()
        block = vbuf[which * group + b].reshape(rows * chans, nx * half)
        turned = jnp.dot(turn_ref[...], block, preferred_element_type=jnp.float32)
        turned = turned.astype(jnp.bfloat16).reshape(CHUNKS, per, rows, nx * half)
        for k in range(nx):
            sbuf[pl.ds(base, CHUNKS), k * group + b] = turned[
                :, :, :, k * half : (k + 1) * half
            ]

    def send_voltage(k, d):
        first = k // CHUNKS * CHUNKS
        skew = k // CHUNKS * (CHUNKS // nx)
        return pltpu.make_async_remote_copy(
            src_ref=sbuf.at[first + lax.rem(k - first + d // group * skew, CHUNKS), d],
            dst_ref=vrecv.at[k, mine],
            send_sem=vsend.at[k],
            recv_sem=vget.at[k],
            device_id=(d // group, side * group + lax.rem(d, group)),
            device_id_type=MESH,
        )

    def keep_voltages(k):
        first = k // CHUNKS * CHUNKS
        skew = k // CHUNKS * (CHUNKS // nx)
        own = sbuf.at[first + lax.rem(k - first + x * skew, CHUNKS), mine]
        pltpu.make_async_copy(own, vrecv.at[k, mine], vget.at[k]).start()

    def send_voltages(k):
        keep_voltages(k)

        def send(i, _):
            send_voltage(k, mine ^ (dests - i)).start()
            return 0

        lax.fori_loop(1, dests, send, 0)

    def send_weights(i):
        span = pl.ds((x * PIECES + i) * piece, piece)
        pltpu.make_async_remote_copy(
            src_ref=w_hbm.at[1 - side, span],
            dst_ref=w_ref.at[1, span],
            send_sem=wsend,
            recv_sem=wz.at[i],
            device_id=(x, partner),
            device_id_type=MESH,
        ).start()

    def relay_weights(i):
        block = w_ref.at[1, pl.ds((x * PIECES + i) * piece, piece)]
        pltpu.make_async_copy(block, block, wz.at[i]).wait()
        pltpu.make_async_remote_copy(
            src_ref=block,
            dst_ref=block,
            send_sem=relay_sem,
            recv_sem=wx.at[i],
            device_id=(1 - x, g),
            device_id_type=MESH,
        ).start()

    pl.semaphore_wait(barrier, dests)
    pl.semaphore_signal(cross, inc=1, device_id=(x, partner), device_id_type=MESH)

    send_weights(0)

    def turn_and_send(i, _):
        @pl.when(i > 0)
        def _():
            b = u ^ (group - i)
            send_voltage(0, (1 - x) * group + b).start()
            send_voltage(0, x * group + b).start()

        turn_block(side, u ^ (group - 1 - i))
        return 0

    lax.fori_loop(0, group, turn_and_send, 0)
    send_voltage(0, (1 - x) * group + u).start()
    keep_voltages(0)
    for k in range(1, CHUNKS):
        send_voltages(k)
        if k % (CHUNKS // PIECES) == 0:
            send_weights(k // (CHUNKS // PIECES))

    def turn(i, _):
        turn_block(1 - side, i)
        return 0

    lax.fori_loop(0, group, turn, 0)
    for k in range(CHUNKS, LEAD):
        send_voltages(k)
    antennas = antennas2 // 2
    i, j = grid_of(mix_ref.shape)
    block = i // antennas
    wants = 2 * (i % antennas) + ((block == 1) | (block == 2)).astype(jnp.int32)
    sign = jnp.where(block == 1, -1.0, 1.0)
    mix_ref[...] = jnp.where(j == wants, sign, 0.0).astype(jnp.bfloat16)
    sample, lane = grid_of(gather_ref.shape[1:])
    for m in range(gather_ref.shape[0]):
        hit = lane == m * (half // 8) + sample // 8
        gather_ref[m] = hit.astype(jnp.float32).astype(jnp.bfloat16)
    w_copy.wait()

    def power_slot(k):
        which = k // CHUNKS
        part_of = lax.rem(k + which * x * (CHUNKS // nx), CHUNKS)
        return codes.at[side, lax.rem(g + which * group, ng), part_of]

    def send_powers(k, d):
        pltpu.make_async_remote_copy(
            src_ref=pbuf.at[k, d],
            dst_ref=power_slot(k),
            send_sem=psend,
            recv_sem=pget.at[k],
            device_id=(x, d),
            device_id_type=MESH,
        ).start()

    def send_near(k):
        pltpu.make_async_copy(pbuf.at[k, g], power_slot(k), pget.at[k]).start()

        def send(i, _):
            send_powers(k, g ^ (group - i))
            return 0

        lax.fori_loop(1, group, send, 0)

    def step(k, _):
        pltpu.make_async_copy(vrecv.at[k], vrecv.at[k], vget.at[k]).wait()

        @pl.when(k + LEAD < steps)
        def _():
            send_voltages(k + LEAD)

        @pl.when((k >= HOLD) & (k < HOLD + PIECES))
        def _():
            relay_weights(k - HOLD)

        for i in range(PIECES):

            @pl.when(k == steps - CHUNKS // nx + i * CHUNKS // nx // PIECES)
            def _(i=i):
                other = w_ref.at[1, pl.ds(((1 - x) * PIECES + i) * piece, piece)]
                pltpu.make_async_copy(other, other, wx.at[i]).wait()

        which = k // CHUNKS
        part_of = lax.rem(k + which * x * (CHUNKS // nx), CHUNKS)

        def channel(c, peak):
            w = w_ref[which, part_of * per + c].reshape(antennas2, beams).T
            power = None
            for h in range(nx):
                v = vrecv[k, h * group : (h + 1) * group, c].reshape(antennas2, half)
                mixed = jnp.dot(mix_ref[...], v, preferred_element_type=jnp.float32)
                mixed = mixed.astype(jnp.bfloat16)
                re = jnp.dot(w, mixed[:antennas2], preferred_element_type=jnp.float32)
                im = jnp.dot(w, mixed[antennas2:], preferred_element_type=jnp.float32)
                part = re * re + im * im
                power = part if power is None else power + part
            own = beams // ng
            packs = own // 8
            power = power.reshape(ng, packs, 8, half)
            total = None
            for m in range(packs):
                p = power[:, m].reshape(ng * 8, half)
                high = p.astype(jnp.bfloat16)
                low = (p - high.astype(jnp.float32)).astype(jnp.bfloat16)
                t = jnp.dot(high, gather_ref[m], preferred_element_type=jnp.float32)
                t += jnp.dot(low, gather_ref[m], preferred_element_type=jnp.float32)
                total = t if total is None else total + t
            total = total.reshape(ng, 8, 128)
            work[:, pl.ds(c, 1)] = total[:, None]
            return jnp.maximum(peak, jnp.max(total, axis=0))

        peak = lax.fori_loop(0, per, channel, jnp.zeros((8, 128), jnp.float32))
        peak = jnp.maximum(jnp.max(peak, keepdims=True), FLOOR)
        code = work[...].reshape(ng, per * 8, 128) * (TOP / peak)[None]
        code = code * code
        code = code * code
        code = code * code
        near = code.astype(jnp.bfloat16).astype(jnp.float32)
        pbuf[k] = jnp.where(code < near, -near, near).astype(jnp.bfloat16)
        row = lax.broadcasted_iota(jnp.int32, peaks.shape, 0)
        lane = lax.broadcasted_iota(jnp.int32, peaks.shape, 1)
        own_row = lax.rem(side + which, 2)
        first = u * chans + part_of * per
        held = (row == own_row) & (lane >= first) & (lane < first + per)
        peaks[...] = jnp.where(held, peak, peaks[...])

        @pl.when(k == 0)
        def _():
            pl.semaphore_wait(cross, 1)

        def send(i, _):
            send_powers(k, (1 - side) * group + i)
            return 0

        @pl.when(side == 0)
        def _():
            send_near(k)

        lax.fori_loop(0, group, send, 0)

        @pl.when(~last & (side == 1))
        def _():
            send_near(k)

        @pl.when(last & (k >= NEAR))
        def _():
            send_near(k - NEAR)

        return 0

    peaks[...] = jnp.zeros_like(peaks)
    lax.fori_loop(0, steps, step, 0)

    pltpu.make_async_copy(peaks, peak_ref.at[side, u], mget).start()

    def send_peaks(i, _):
        pltpu.make_async_remote_copy(
            src_ref=peaks,
            dst_ref=peak_ref.at[side, u],
            send_sem=msend,
            recv_sem=mget,
            device_id=(x, lax.rem(g + i, ng)),
            device_id_type=MESH,
        ).start()
        return 0

    lax.fori_loop(1, ng, send_peaks, 0)

    @pl.when(last)
    def _():
        def late(k, _):
            send_near(k)
            return 0

        lax.fori_loop(steps - NEAR, steps, late, 0)

    def decode(k, _):
        pltpu.make_async_copy(pbuf.at[k], pbuf.at[k], pget.at[k]).wait()
        which = k // CHUNKS
        part_of = lax.rem(k + which * x * (CHUNKS // nx), CHUNKS)
        for other in range(2):
            span = pl.ds((other + which) % 2 * group, group)
            code = codes[other, span, part_of].astype(jnp.float32)
            near = jnp.abs(code)
            gap = (near * NEXT).astype(jnp.bfloat16).astype(jnp.float32) - near
            near = near + jnp.where(code < 0, -0.25, 0.25) * gap
            plain[other, span, part_of] = jnp.exp(jnp.log(near) * 0.125)
            pltpu.make_async_copy(
                plain.at[other, span, part_of],
                out_ref.at[other, span, part_of],
                out_sem,
            ).start()
        return 0

    lax.fori_loop(0, steps, decode, 0)
    pltpu.make_async_copy(peak_ref, peak_ref, mget).wait()
    pltpu.make_async_copy(out_ref, out_ref, out_sem).wait()
    for k in range(steps):
        sent = sbuf.at[k, pl.ds(0, dests - 1)]
        pltpu.make_async_copy(sent, sent, vsend.at[k]).wait()
    sent = pbuf.at[:, pl.ds(0, ng - 1)]
    pltpu.make_async_copy(sent, sent, psend).wait()
    sent = peak_ref.at[:, pl.ds(0, group - 1)]
    pltpu.make_async_copy(sent, sent, msend).wait()
    sent = peak_ref.at[0, pl.ds(0, 1)]
    pltpu.make_async_copy(sent, sent, msend).wait()
    sent = w_ref.at[1, pl.ds(0, PIECES * piece)]
    pltpu.make_async_copy(sent, sent, wsend).wait()
    pltpu.make_async_copy(sent, sent, relay_sem).wait()


def spread_kernel(in_ref, peak_ref, out_ref, block, sem):
    channels, bins = out_ref.shape[3], out_ref.shape[2]
    packs = 128 // bins

    def copies(q, r):
        for m in range(packs):
            yield pltpu.make_async_copy(block.at[q, m * 8 + r], out_ref.at[q, m * 8 + r], sem)

    before = None
    for q in range(2):
        scale = jnp.sum(peak_ref[q], axis=0) * (1.0 / TOP)
        scale = jnp.concatenate([scale[0:1], scale[1:2]], axis=1)
        for r in range(8):
            lanes = in_ref[q, pl.ds(r, channels, stride=8), :].T * scale
            for m in range(packs):
                block[q, m * 8 + r] = lanes[m * bins : (m + 1) * bins]
            if before is not None:
                for copy in copies(*before):
                    copy.start()
            before = (q, r)
    for copy in copies(*before):
        copy.start()
    pltpu.make_async_copy(block, out_ref, sem).wait()


def on_device(nx, ng, voltages, weights):
    v = voltages[0]
    streams, parts, channels, samples = v.shape
    rows, chans, half = streams * parts, channels // ng, samples // nx
    per = chans // CHUNKS
    group = ng // 2
    antennas = group * streams
    beams = weights.shape[3]
    own = beams // ng
    packs = own // 8
    bins = half // 8

    turned_weights = jnp.swapaxes(weights, 3, 4)
    hbm = pl.BlockSpec(memory_space=pltpu.HBM)
    anywhere = pl.BlockSpec(memory_space=pl.ANY)
    packed, peaks = pl.pallas_call(
        functools.partial(kernel, nx, ng),
        out_shape=(
            jax.ShapeDtypeStruct((2, ng, CHUNKS, per * 8, 128), jnp.float32),
            jax.ShapeDtypeStruct((2, group, 2, 128), jnp.float32),
        ),
        in_specs=[hbm, hbm],
        out_specs=(anywhere, anywhere),
        scratch_shapes=[
            pltpu.VMEM((rows * chans, rows * chans), jnp.bfloat16),
            pltpu.VMEM((4 * antennas, 2 * antennas), jnp.bfloat16),
            pltpu.VMEM((packs, half, 128), jnp.bfloat16),
            pltpu.VMEM((2 * group, streams, parts, chans, samples), jnp.bfloat16),
            pltpu.VMEM((2 * CHUNKS, nx * group, per, rows, half), jnp.bfloat16),
            pltpu.VMEM((2 * CHUNKS, nx * group, per, rows, half), jnp.bfloat16),
            pltpu.VMEM(turned_weights.shape, jnp.bfloat16),
            pltpu.VMEM((ng, per, 8, 128), jnp.float32),
            pltpu.VMEM((2 * CHUNKS, ng, per * 8, 128), jnp.bfloat16),
            pltpu.VMEM((2, ng, CHUNKS, per * 8, 128), jnp.bfloat16),
            pltpu.VMEM((2, ng, CHUNKS, per * 8, 128), jnp.float32),
            pltpu.VMEM((2, 128), jnp.float32),
            pltpu.SemaphoreType.DMA((2 * group,)),
            pltpu.SemaphoreType.REGULAR,
            pltpu.SemaphoreType.DMA,
            pltpu.SemaphoreType.DMA,
            pltpu.SemaphoreType.DMA((PIECES,)),
            pltpu.SemaphoreType.DMA,
            pltpu.SemaphoreType.DMA((PIECES,)),
            pltpu.SemaphoreType.DMA((2 * CHUNKS,)),
            pltpu.SemaphoreType.DMA((2 * CHUNKS,)),
            pltpu.SemaphoreType.DMA,
            pltpu.SemaphoreType.DMA((2 * CHUNKS,)),
            pltpu.SemaphoreType.DMA,
            pltpu.SemaphoreType.DMA,
            pltpu.SemaphoreType.DMA,
        ],
        compiler_params=pltpu.CompilerParams(
            collective_id=0, has_side_effects=True, vmem_limit_bytes=VMEM
        ),
    )(v, turned_weights)

    spread = pl.pallas_call(
        spread_kernel,
        out_shape=jax.ShapeDtypeStruct((2, own, bins, channels), jnp.float32),
        in_specs=[pl.BlockSpec(memory_space=pltpu.VMEM)] * 2,
        out_specs=anywhere,
        scratch_shapes=[
            pltpu.VMEM((2, own, bins, channels), jnp.float32),
            pltpu.SemaphoreType.DMA,
        ],
        compiler_params=pltpu.CompilerParams(vmem_limit_bytes=VMEM),
    )(packed.reshape(2, channels * 8, 128), peaks)
    return spread.transpose(3, 0, 1, 2)


def solution(mesh):
    nx, ng = mesh.shape["ta"], mesh.shape["gx"]

    def body(voltages, weights):
        _, streams, parts, channels, samples = voltages.shape
        rows, chans, half = streams * parts, channels // ng, samples // nx
        own = weights.shape[3] // ng
        fits = (
            nx == 2
            and rows % 16 == 0
            and chans % 16 == 0
            and half % 128 == 0
            and own % 8 == 0
            and (own // 8) * (half // 8) == 128
            and ng % 2 == 0
            and ng & (ng - 1) == 0
            and ng * chans == 256
        )
        if fits:
            return on_device(nx, ng, voltages, weights)
        return plain_on_device(voltages, weights)

    in_specs = (P("ta", "gx", None, None, None), P(None, "gx", None, None, None))
    out_specs = P(None, None, "gx", "ta")
    return jax.shard_map(
        body, mesh=mesh, in_specs=in_specs, out_specs=out_specs, check_vma=False
    )
```

```python
import functools

import jax
import jax.numpy as jnp
from jax import lax
from jax.experimental import pallas as pl
from jax.experimental.pallas import tpu as pltpu
from jax.sharding import PartitionSpec as P

MESH = pl.DeviceIdType.MESH
VMEM = 48 * 1024 * 1024
CHUNKS = 8
PIECES = 4
HOLD = 2
LEAD = 16
NEAR = 6
TOP = 2.0**15.75
FLOOR = 2.0**-90
NEXT = 1.0 + 1.3 / 256


def beam_power(voltage, weight_block):
    antennas = weight_block.shape[3]
    beam_count = weight_block.shape[2]
    powers = []
    for side_index in range(2):
        real_w = weight_block[side_index, 0]
        imag_w = weight_block[side_index, 1]
        upper_rows = jnp.stack([real_w, -imag_w], axis=-1).reshape(beam_count, 2 * antennas)
        bottom_half_rows = jnp.stack([imag_w, real_w], axis=-1).reshape(beam_count, 2 * antennas)
        matrix = jnp.concatenate([upper_rows, bottom_half_rows], 0)
        signal = voltage[side_index * antennas : (side_index + 1) * antennas].reshape(
            2 * antennas, -1
        )
        beam_voltage_field = jnp.dot(matrix, signal, preferred_element_type=jnp.float32)
        power = (
            beam_voltage_field[:beam_count] * beam_voltage_field[:beam_count]
            + beam_voltage_field[beam_count:] * beam_voltage_field[beam_count:]
        )
        powers.append(power.reshape(beam_count, -1, 8).sum(-1))
    return jnp.stack(powers, 0)


def channel_powers(turned, weights):

    def one_channel(column):
        voltage = lax.dynamic_index_in_dim(turned, column, 2, keepdims=False)
        weight_block = lax.dynamic_index_in_dim(weights, column, 1, keepdims=False)
        return beam_power(voltage, weight_block)

    return lax.map(one_channel, jnp.arange(turned.shape[2], dtype=jnp.int32))


def plain_on_device(voltages, weights):
    turned = lax.all_to_all(voltages, "gx", split_axis=3, concat_axis=1, tiled=True)
    partial_power_value = channel_powers(turned[0], weights)
    relaid = lax.all_to_all(partial_power_value, "gx", split_axis=2, concat_axis=0, tiled=True)
    return lax.psum_scatter(relaid, "ta", scatter_dimension=3, tiled=True)


def kernel(
    nx, ng, v_hbm, w_hbm, out_ref, peak_ref,
    turn_ref, mix_ref, gather_ref, vbuf, sbuf, vrecv, w_ref, work, pbuf, codes, plain, peaks,
    v_sem, cross, w_sem, wsend, wz, relay_sem, wx, vsend, vget, psend, pget, msend, mget, out_sem,
):
    x = lax.axis_index("ta")
    g = lax.axis_index("gx")
    rows = v_hbm.shape[0] * v_hbm.shape[1]
    chans = v_hbm.shape[2] // ng
    half = v_hbm.shape[3] // nx
    per = chans // CHUNKS
    group = ng // 2
    antennas2 = group * rows
    beams = w_ref.shape[4]
    side = g // group
    u = lax.rem(g, group)
    partner = lax.rem(g + group, ng)
    last = (side == 1) & (u >= group // 2)
    steps = 2 * CHUNKS
    dests = nx * group
    mine = x * group + u
    piece = chans // nx // PIECES

    barrier = pltpu.get_barrier_semaphore()

    def greet(i, _):
        d = mine ^ i
        pl.semaphore_signal(
            barrier,
            inc=1,
            device_id=(d // group, side * group + lax.rem(d, group)),
            device_id_type=MESH,
        )
        return 0

    lax.fori_loop(1, dests, greet, 0)
    pl.semaphore_signal(barrier, inc=1, device_id=(x, partner), device_id_type=MESH)

    w_copy = pltpu.make_async_copy(w_hbm.at[side], w_ref.at[0], w_sem)

    def fetch(block):
        return pltpu.make_async_copy(
            v_hbm.at[:, :, pl.ds(pl.multiple_of(block * chans, chans), chans), :],
            vbuf.at[block],
            v_sem.at[block],
        )

    def fetch_side(which):
        def start(i, _):
            fetch(which * group + (u ^ (group - 1 - i))).start()
            return 0

        lax.fori_loop(0, group, start, 0)

    fetch_side(side)

    def grid_of(shape):
        return [lax.broadcasted_iota(jnp.int32, shape, axis) for axis in (0, 1)]

    i, j = grid_of(turn_ref.shape)
    hit = (j % chans == i // rows) & (j // chans == i % rows)
    turn_ref[...] = hit.astype(jnp.float32).astype(jnp.bfloat16)

    def turn_block(which, b):
        base = lax.rem(which + side, 2) * CHUNKS
        fetch(which * group + b).wait()
        block = vbuf[which * group + b].reshape(rows * chans, nx * half)
        turned = jnp.dot(turn_ref[...], block, preferred_element_type=jnp.float32)
        turned = turned.astype(jnp.bfloat16).reshape(CHUNKS, per, rows, nx * half)
        for k in range(nx):
            sbuf[pl.ds(base, CHUNKS), k * group + b] = turned[
                :, :, :, k * half : (k + 1) * half
            ]

    def send_voltage(k, d):
        first = k // CHUNKS * CHUNKS
        skew = k // CHUNKS * (CHUNKS // nx)
        return pltpu.make_async_remote_copy(
            src_ref=sbuf.at[first + lax.rem(k - first + d // group * skew, CHUNKS), d],
            dst_ref=vrecv.at[k, mine],
            send_sem=vsend.at[k],
            recv_sem=vget.at[k],
            device_id=(d // group, side * group + lax.rem(d, group)),
            device_id_type=MESH,
        )

    def keep_voltages(k):
        first = k // CHUNKS * CHUNKS
        skew = k // CHUNKS * (CHUNKS // nx)
        own = sbuf.at[first + lax.rem(k - first + x * skew, CHUNKS), mine]
        pltpu.make_async_copy(own, vrecv.at[k, mine], vget.at[k]).start()

    def send_voltages(k):
        keep_voltages(k)

        def send(i, _):
            send_voltage(k, mine ^ (dests - i)).start()
            return 0

        lax.fori_loop(1, dests, send, 0)

    def send_weights(i):
        span = pl.ds((x * PIECES + i) * piece, piece)
        pltpu.make_async_remote_copy(
            src_ref=w_hbm.at[1 - side, span],
            dst_ref=w_ref.at[1, span],
            send_sem=wsend,
            recv_sem=wz.at[i],
            device_id=(x, partner),
            device_id_type=MESH,
        ).start()

    def relay_weights(i):
        block = w_ref.at[1, pl.ds((x * PIECES + i) * piece, piece)]
        pltpu.make_async_copy(block, block, wz.at[i]).wait()
        pltpu.make_async_remote_copy(
            src_ref=block,
            dst_ref=block,
            send_sem=relay_sem,
            recv_sem=wx.at[i],
            device_id=(1 - x, g),
            device_id_type=MESH,
        ).start()

    pl.semaphore_wait(barrier, dests)
    pl.semaphore_signal(cross, inc=1, device_id=(x, partner), device_id_type=MESH)

    send_weights(0)

    def turn_and_send(i, _):
        @pl.when(i > 0)
        def _():
            b = u ^ (group - i)
            send_voltage(0, (1 - x) * group + b).start()
            send_voltage(0, x * group + b).start()

        turn_block(side, u ^ (group - 1 - i))
        return 0

    lax.fori_loop(0, group, turn_and_send, 0)
    fetch_side(1 - side)
    w_copy.start()
    send_voltage(0, (1 - x) * group + u).start()
    keep_voltages(0)
    for k in range(1, CHUNKS):
        send_voltages(k)
        if k % (CHUNKS // PIECES) == 0:
            send_weights(k // (CHUNKS // PIECES))

    def turn(i, _):
        turn_block(1 - side, i)
        return 0

    lax.fori_loop(0, group, turn, 0)
    for k in range(CHUNKS, LEAD):
        send_voltages(k)
    antennas = antennas2 // 2
    i, j = grid_of(mix_ref.shape)
    block = i // antennas
    wants = 2 * (i % antennas) + ((block == 1) | (block == 2)).astype(jnp.int32)
    sign = jnp.where(block == 1, -1.0, 1.0)
    mix_ref[...] = jnp.where(j == wants, sign, 0.0).astype(jnp.bfloat16)
    sample, lane = grid_of(gather_ref.shape[1:])
    for m in range(gather_ref.shape[0]):
        hit = lane == m * (half // 8) + sample // 8
        gather_ref[m] = hit.astype(jnp.float32).astype(jnp.bfloat16)
    w_copy.wait()

    def power_slot(k):
        which = k // CHUNKS
        part_of = lax.rem(k + which * x * (CHUNKS // nx), CHUNKS)
        return codes.at[side, lax.rem(g + which * group, ng), part_of]

    def send_powers(k, d):
        pltpu.make_async_remote_copy(
            src_ref=pbuf.at[k, d],
            dst_ref=power_slot(k),
            send_sem=psend,
            recv_sem=pget.at[k],
            device_id=(x, d),
            device_id_type=MESH,
        ).start()

    def send_near(k):
        pltpu.make_async_copy(pbuf.at[k, g], power_slot(k), pget.at[k]).start()

        def send(i, _):
            send_powers(k, g ^ (group - i))
            return 0

        lax.fori_loop(1, group, send, 0)

    def step(k, _):
        pltpu.make_async_copy(vrecv.at[k], vrecv.at[k], vget.at[k]).wait()

        @pl.when(k + LEAD < steps)
        def _():
            send_voltages(k + LEAD)

        @pl.when((k >= HOLD) & (k < HOLD + PIECES))
        def _():
            relay_weights(k - HOLD)

        for i in range(PIECES):

            @pl.when(k == steps - CHUNKS // nx + i * CHUNKS // nx // PIECES)
            def _(i=i):
                other = w_ref.at[1, pl.ds(((1 - x) * PIECES + i) * piece, piece)]
                pltpu.make_async_copy(other, other, wx.at[i]).wait()

        which = k // CHUNKS
        part_of = lax.rem(k + which * x * (CHUNKS // nx), CHUNKS)

        def channel(c, peak):
            w = w_ref[which, part_of * per + c].reshape(antennas2, beams).T
            power = None
            for h in range(nx):
                v = vrecv[k, h * group : (h + 1) * group, c].reshape(antennas2, half)
                mixed = jnp.dot(mix_ref[...], v, preferred_element_type=jnp.float32)
                mixed = mixed.astype(jnp.bfloat16)
                re = jnp.dot(w, mixed[:antennas2], preferred_element_type=jnp.float32)
                im = jnp.dot(w, mixed[antennas2:], preferred_element_type=jnp.float32)
                part = re * re + im * im
                power = part if power is None else power + part
            own = beams // ng
            packs = own // 8
            power = power.reshape(ng, packs, 8, half)
            total = None
            for m in range(packs):
                p = power[:, m].reshape(ng * 8, half)
                high = p.astype(jnp.bfloat16)
                low = (p - high.astype(jnp.float32)).astype(jnp.bfloat16)
                t = jnp.dot(high, gather_ref[m], preferred_element_type=jnp.float32)
                t += jnp.dot(low, gather_ref[m], preferred_element_type=jnp.float32)
                total = t if total is None else total + t
            total = total.reshape(ng, 8, 128)
            work[:, pl.ds(c, 1)] = total[:, None]
            return jnp.maximum(peak, jnp.max(total, axis=0))

        peak = lax.fori_loop(0, per, channel, jnp.zeros((8, 128), jnp.float32))
        peak = jnp.maximum(jnp.max(peak, keepdims=True), FLOOR)
        code = work[...].reshape(ng, per * 8, 128) * (TOP / peak)[None]
        code = code * code
        code = code * code
        code = code * code
        near = code.astype(jnp.bfloat16).astype(jnp.float32)
        pbuf[k] = jnp.where(code < near, -near, near).astype(jnp.bfloat16)
        row = lax.broadcasted_iota(jnp.int32, peaks.shape, 0)
        lane = lax.broadcasted_iota(jnp.int32, peaks.shape, 1)
        own_row = lax.rem(side + which, 2)
        first = u * chans + part_of * per
        held = (row == own_row) & (lane >= first) & (lane < first + per)
        peaks[...] = jnp.where(held, peak, peaks[...])

        @pl.when(k == 0)
        def _():
            pl.semaphore_wait(cross, 1)

        def send(i, _):
            send_powers(k, (1 - side) * group + i)
            return 0

        @pl.when(side == 0)
        def _():
            send_near(k)

        lax.fori_loop(0, group, send, 0)

        @pl.when(~last & (side == 1))
        def _():
            send_near(k)

        @pl.when(last & (k >= NEAR))
        def _():
            send_near(k - NEAR)

        return 0

    peaks[...] = jnp.zeros_like(peaks)
    lax.fori_loop(0, steps, step, 0)

    pltpu.make_async_copy(peaks, peak_ref.at[side, u], mget).start()

    def send_peaks(i, _):
        pltpu.make_async_remote_copy(
            src_ref=peaks,
            dst_ref=peak_ref.at[side, u],
            send_sem=msend,
            recv_sem=mget,
            device_id=(x, lax.rem(g + i, ng)),
            device_id_type=MESH,
        ).start()
        return 0

    lax.fori_loop(1, ng, send_peaks, 0)

    @pl.when(last)
    def _():
        def late(k, _):
            send_near(k)
            return 0

        lax.fori_loop(steps - NEAR, steps, late, 0)

    def decode(k, _):
        pltpu.make_async_copy(pbuf.at[k], pbuf.at[k], pget.at[k]).wait()
        which = k // CHUNKS
        part_of = lax.rem(k + which * x * (CHUNKS // nx), CHUNKS)
        for other in range(2):
            span = pl.ds((other + which) % 2 * group, group)
            code = codes[other, span, part_of].astype(jnp.float32)
            near = jnp.abs(code)
            gap = (near * NEXT).astype(jnp.bfloat16).astype(jnp.float32) - near
            near = near + jnp.where(code < 0, -0.25, 0.25) * gap
            plain[other, span, part_of] = jnp.exp(jnp.log(near) * 0.125)
            pltpu.make_async_copy(
                plain.at[other, span, part_of],
                out_ref.at[other, span, part_of],
                out_sem,
            ).start()
        return 0

    lax.fori_loop(0, steps, decode, 0)
    pltpu.make_async_copy(peak_ref, peak_ref, mget).wait()
    pltpu.make_async_copy(out_ref, out_ref, out_sem).wait()
    for k in range(steps):
        sent = sbuf.at[k, pl.ds(0, dests - 1)]
        pltpu.make_async_copy(sent, sent, vsend.at[k]).wait()
    sent = pbuf.at[:, pl.ds(0, ng - 1)]
    pltpu.make_async_copy(sent, sent, psend).wait()
    sent = peak_ref.at[:, pl.ds(0, group - 1)]
    pltpu.make_async_copy(sent, sent, msend).wait()
    sent = peak_ref.at[0, pl.ds(0, 1)]
    pltpu.make_async_copy(sent, sent, msend).wait()
    sent = w_ref.at[1, pl.ds(0, PIECES * piece)]
    pltpu.make_async_copy(sent, sent, wsend).wait()
    pltpu.make_async_copy(sent, sent, relay_sem).wait()


def spread_kernel(in_ref, peak_ref, out_ref, block, sem):
    channels, bins = out_ref.shape[3], out_ref.shape[2]
    packs = 128 // bins

    def copies(q, r):
        for m in range(packs):
            yield pltpu.make_async_copy(block.at[q, m * 8 + r], out_ref.at[q, m * 8 + r], sem)

    before = None
    for q in range(2):
        scale = jnp.sum(peak_ref[q], axis=0) * (1.0 / TOP)
        scale = jnp.concatenate([scale[0:1], scale[1:2]], axis=1)
        for r in range(8):
            lanes = in_ref[q, pl.ds(r, channels, stride=8), :].T * scale
            for m in range(packs):
                block[q, m * 8 + r] = lanes[m * bins : (m + 1) * bins]
            if before is not None:
                for copy in copies(*before):
                    copy.start()
            before = (q, r)
    for copy in copies(*before):
        copy.start()
    pltpu.make_async_copy(block, out_ref, sem).wait()


def on_device(nx, ng, voltages, weights):
    v = voltages[0]
    streams, parts, channels, samples = v.shape
    rows, chans, half = streams * parts, channels // ng, samples // nx
    per = chans // CHUNKS
    group = ng // 2
    antennas = group * streams
    beams = weights.shape[3]
    own = beams // ng
    packs = own // 8
    bins = half // 8

    turned_weights = jnp.swapaxes(weights, 3, 4)
    hbm = pl.BlockSpec(memory_space=pltpu.HBM)
    anywhere = pl.BlockSpec(memory_space=pl.ANY)
    packed, peaks = pl.pallas_call(
        functools.partial(kernel, nx, ng),
        out_shape=(
            jax.ShapeDtypeStruct((2, ng, CHUNKS, per * 8, 128), jnp.float32),
            jax.ShapeDtypeStruct((2, group, 2, 128), jnp.float32),
        ),
        in_specs=[hbm, hbm],
        out_specs=(anywhere, anywhere),
        scratch_shapes=[
            pltpu.VMEM((rows * chans, rows * chans), jnp.bfloat16),
            pltpu.VMEM((4 * antennas, 2 * antennas), jnp.bfloat16),
            pltpu.VMEM((packs, half, 128), jnp.bfloat16),
            pltpu.VMEM((2 * group, streams, parts, chans, samples), jnp.bfloat16),
            pltpu.VMEM((2 * CHUNKS, nx * group, per, rows, half), jnp.bfloat16),
            pltpu.VMEM((2 * CHUNKS, nx * group, per, rows, half), jnp.bfloat16),
            pltpu.VMEM(turned_weights.shape, jnp.bfloat16),
            pltpu.VMEM((ng, per, 8, 128), jnp.float32),
            pltpu.VMEM((2 * CHUNKS, ng, per * 8, 128), jnp.bfloat16),
            pltpu.VMEM((2, ng, CHUNKS, per * 8, 128), jnp.bfloat16),
            pltpu.VMEM((2, ng, CHUNKS, per * 8, 128), jnp.float32),
            pltpu.VMEM((2, 128), jnp.float32),
            pltpu.SemaphoreType.DMA((2 * group,)),
            pltpu.SemaphoreType.REGULAR,
            pltpu.SemaphoreType.DMA,
            pltpu.SemaphoreType.DMA,
            pltpu.SemaphoreType.DMA((PIECES,)),
            pltpu.SemaphoreType.DMA,
            pltpu.SemaphoreType.DMA((PIECES,)),
            pltpu.SemaphoreType.DMA((2 * CHUNKS,)),
            pltpu.SemaphoreType.DMA((2 * CHUNKS,)),
            pltpu.SemaphoreType.DMA,
            pltpu.SemaphoreType.DMA((2 * CHUNKS,)),
            pltpu.SemaphoreType.DMA,
            pltpu.SemaphoreType.DMA,
            pltpu.SemaphoreType.DMA,
        ],
        compiler_params=pltpu.CompilerParams(
            collective_id=0, has_side_effects=True, vmem_limit_bytes=VMEM
        ),
    )(v, turned_weights)

    spread = pl.pallas_call(
        spread_kernel,
        out_shape=jax.ShapeDtypeStruct((2, own, bins, channels), jnp.float32),
        in_specs=[pl.BlockSpec(memory_space=pltpu.VMEM)] * 2,
        out_specs=anywhere,
        scratch_shapes=[
            pltpu.VMEM((2, own, bins, channels), jnp.float32),
            pltpu.SemaphoreType.DMA,
        ],
        compiler_params=pltpu.CompilerParams(vmem_limit_bytes=VMEM),
    )(packed.reshape(2, channels * 8, 128), peaks)
    return spread.transpose(3, 0, 1, 2)


def solution(mesh):
    nx, ng = mesh.shape["ta"], mesh.shape["gx"]

    def body(voltages, weights):
        _, streams, parts, channels, samples = voltages.shape
        rows, chans, half = streams * parts, channels // ng, samples // nx
        own = weights.shape[3] // ng
        fits = (
            nx == 2
            and rows % 16 == 0
            and chans % 16 == 0
            and half % 128 == 0
            and own % 8 == 0
            and (own // 8) * (half // 8) == 128
            and ng % 2 == 0
            and ng & (ng - 1) == 0
            and ng * chans == 256
        )
        if fits:
            return on_device(nx, ng, voltages, weights)
        return plain_on_device(voltages, weights)

    in_specs = (P("ta", "gx", None, None, None), P(None, "gx", None, None, None))
    out_specs = P(None, None, "gx", "ta")
    return jax.shard_map(
        body, mesh=mesh, in_specs=in_specs, out_specs=out_specs, check_vma=False
    )
```

```python
import functools

import jax
import jax.numpy as jnp
from jax import lax
from jax.experimental import pallas as pl
from jax.experimental.pallas import tpu as pltpu
from jax.sharding import PartitionSpec as P

MESH = pl.DeviceIdType.MESH
VMEM = 48 * 1024 * 1024
CHUNKS = 8
PIECES = 4
HOLD = 2
LEAD = 16
NEAR = 6
TOP = 2.0**15.75
FLOOR = 2.0**-90
NEXT = 1.0 + 1.3 / 256


def beam_power(voltage, weight_block):
    antennas = weight_block.shape[3]
    beam_count = weight_block.shape[2]
    powers = []
    for side_index in range(2):
        real_w = weight_block[side_index, 0]
        imag_w = weight_block[side_index, 1]
        upper_rows = jnp.stack([real_w, -imag_w], axis=-1).reshape(beam_count, 2 * antennas)
        bottom_half_rows = jnp.stack([imag_w, real_w], axis=-1).reshape(beam_count, 2 * antennas)
        matrix = jnp.concatenate([upper_rows, bottom_half_rows], 0)
        signal = voltage[side_index * antennas : (side_index + 1) * antennas].reshape(
            2 * antennas, -1
        )
        beam_voltage_field = jnp.dot(matrix, signal, preferred_element_type=jnp.float32)
        power = (
            beam_voltage_field[:beam_count] * beam_voltage_field[:beam_count]
            + beam_voltage_field[beam_count:] * beam_voltage_field[beam_count:]
        )
        powers.append(power.reshape(beam_count, -1, 8).sum(-1))
    return jnp.stack(powers, 0)


def channel_powers(turned, weights):

    def one_channel(column):
        voltage = lax.dynamic_index_in_dim(turned, column, 2, keepdims=False)
        weight_block = lax.dynamic_index_in_dim(weights, column, 1, keepdims=False)
        return beam_power(voltage, weight_block)

    return lax.map(one_channel, jnp.arange(turned.shape[2], dtype=jnp.int32))


def plain_on_device(voltages, weights):
    turned = lax.all_to_all(voltages, "gx", split_axis=3, concat_axis=1, tiled=True)
    partial_power_value = channel_powers(turned[0], weights)
    relaid = lax.all_to_all(partial_power_value, "gx", split_axis=2, concat_axis=0, tiled=True)
    return lax.psum_scatter(relaid, "ta", scatter_dimension=3, tiled=True)


def kernel(
    nx, ng, v_hbm, w_hbm, out_ref, peak_ref,
    turn_ref, mix_ref, gather_ref, vbuf, sbuf, vrecv, w_ref, work, pbuf, codes, plain, peaks,
    v_sem, cross, w_sem, wsend, wz, relay_sem, wx, vsend, vget, psend, pget, msend, mget, out_sem,
):
    x = lax.axis_index("ta")
    g = lax.axis_index("gx")
    rows = v_hbm.shape[0] * v_hbm.shape[1]
    chans = v_hbm.shape[2] // ng
    half = v_hbm.shape[3] // nx
    per = chans // CHUNKS
    group = ng // 2
    antennas2 = group * rows
    beams = w_ref.shape[4]
    side = g // group
    u = lax.rem(g, group)
    partner = lax.rem(g + group, ng)
    last = (side == 1) & (u >= group // 2)
    steps = 2 * CHUNKS
    dests = nx * group
    mine = x * group + u
    piece = chans // nx // PIECES

    barrier = pltpu.get_barrier_semaphore()

    def greet(i, _):
        d = mine ^ i
        pl.semaphore_signal(
            barrier,
            inc=1,
            device_id=(d // group, side * group + lax.rem(d, group)),
            device_id_type=MESH,
        )
        return 0

    lax.fori_loop(1, dests, greet, 0)
    pl.semaphore_signal(barrier, inc=1, device_id=(x, partner), device_id_type=MESH)

    w_copy = pltpu.make_async_copy(w_hbm.at[side], w_ref.at[0], w_sem)

    def fetch(block):
        return pltpu.make_async_copy(
            v_hbm.at[:, :, pl.ds(pl.multiple_of(block * chans, chans), chans), :],
            vbuf.at[block],
            v_sem.at[block],
        )

    def fetch_side(which):
        def start(i, _):
            fetch(which * group + (u ^ (group - 1 - i))).start()
            return 0

        lax.fori_loop(0, group, start, 0)

    fetch_side(side)

    def grid_of(shape):
        return [lax.broadcasted_iota(jnp.int32, shape, axis) for axis in (0, 1)]


    def turn_block(which, b):
        base = lax.rem(which + side, 2) * CHUNKS
        fetch(which * group + b).wait()
        block = vbuf[which * group + b].reshape(rows * chans, nx * half)
        turned = jnp.dot(turn_ref[...], block, preferred_element_type=jnp.float32)
        turned = turned.astype(jnp.bfloat16).reshape(CHUNKS, per, rows, nx * half)
        for k in range(nx):
            sbuf[pl.ds(base, CHUNKS), k * group + b] = turned[
                :, :, :, k * half : (k + 1) * half
            ]

    def send_voltage(k, d):
        first = k // CHUNKS * CHUNKS
        skew = k // CHUNKS * (CHUNKS // nx)
        return pltpu.make_async_remote_copy(
            src_ref=sbuf.at[first + lax.rem(k - first + d // group * skew, CHUNKS), d],
            dst_ref=vrecv.at[k, mine],
            send_sem=vsend.at[k],
            recv_sem=vget.at[k],
            device_id=(d // group, side * group + lax.rem(d, group)),
            device_id_type=MESH,
        )

    def keep_voltages(k):
        first = k // CHUNKS * CHUNKS
        skew = k // CHUNKS * (CHUNKS // nx)
        own = sbuf.at[first + lax.rem(k - first + x * skew, CHUNKS), mine]
        pltpu.make_async_copy(own, vrecv.at[k, mine], vget.at[k]).start()

    def send_voltages(k):
        keep_voltages(k)

        def send(i, _):
            send_voltage(k, mine ^ (dests - i)).start()
            return 0

        lax.fori_loop(1, dests, send, 0)

    def send_weights(i):
        span = pl.ds((x * PIECES + i) * piece, piece)
        pltpu.make_async_remote_copy(
            src_ref=w_hbm.at[1 - side, span],
            dst_ref=w_ref.at[1, span],
            send_sem=wsend,
            recv_sem=wz.at[i],
            device_id=(x, partner),
            device_id_type=MESH,
        ).start()

    def relay_weights(i):
        block = w_ref.at[1, pl.ds((x * PIECES + i) * piece, piece)]
        pltpu.make_async_copy(block, block, wz.at[i]).wait()
        pltpu.make_async_remote_copy(
            src_ref=block,
            dst_ref=block,
            send_sem=relay_sem,
            recv_sem=wx.at[i],
            device_id=(1 - x, g),
            device_id_type=MESH,
        ).start()

    pl.semaphore_wait(barrier, dests)
    pl.semaphore_signal(cross, inc=1, device_id=(x, partner), device_id_type=MESH)

    send_weights(0)
    i, j = grid_of(turn_ref.shape)
    hit = (j % chans == i // rows) & (j // chans == i % rows)
    turn_ref[...] = hit.astype(jnp.float32).astype(jnp.bfloat16)

    def turn_and_send(i, _):
        @pl.when(i > 0)
        def _():
            b = u ^ (group - i)
            send_voltage(0, (1 - x) * group + b).start()
            send_voltage(0, x * group + b).start()

        turn_block(side, u ^ (group - 1 - i))
        return 0

    lax.fori_loop(0, group, turn_and_send, 0)
    fetch_side(1 - side)
    w_copy.start()
    send_voltage(0, (1 - x) * group + u).start()
    keep_voltages(0)
    for k in range(1, CHUNKS):
        send_voltages(k)
        if k % (CHUNKS // PIECES) == 0:
            send_weights(k // (CHUNKS // PIECES))

    def turn(i, _):
        turn_block(1 - side, i)
        return 0

    lax.fori_loop(0, group, turn, 0)
    for k in range(CHUNKS, LEAD):
        send_voltages(k)
    antennas = antennas2 // 2
    i, j = grid_of(mix_ref.shape)
    block = i // antennas
    wants = 2 * (i % antennas) + ((block == 1) | (block == 2)).astype(jnp.int32)
    sign = jnp.where(block == 1, -1.0, 1.0)
    mix_ref[...] = jnp.where(j == wants, sign, 0.0).astype(jnp.bfloat16)
    sample, lane = grid_of(gather_ref.shape[1:])
    for m in range(gather_ref.shape[0]):
        hit = lane == m * (half // 8) + sample // 8
        gather_ref[m] = hit.astype(jnp.float32).astype(jnp.bfloat16)
    w_copy.wait()

    def power_slot(k):
        which = k // CHUNKS
        part_of = lax.rem(k + which * x * (CHUNKS // nx), CHUNKS)
        return codes.at[side, lax.rem(g + which * group, ng), part_of]

    def send_powers(k, d):
        pltpu.make_async_remote_copy(
            src_ref=pbuf.at[k, d],
            dst_ref=power_slot(k),
            send_sem=psend,
            recv_sem=pget.at[k],
            device_id=(x, d),
            device_id_type=MESH,
        ).start()

    def send_near(k):
        pltpu.make_async_copy(pbuf.at[k, g], power_slot(k), pget.at[k]).start()

        def send(i, _):
            send_powers(k, g ^ (group - i))
            return 0

        lax.fori_loop(1, group, send, 0)

    def step(k, _):
        pltpu.make_async_copy(vrecv.at[k], vrecv.at[k], vget.at[k]).wait()

        @pl.when(k + LEAD < steps)
        def _():
            send_voltages(k + LEAD)

        @pl.when((k >= HOLD) & (k < HOLD + PIECES))
        def _():
            relay_weights(k - HOLD)

        for i in range(PIECES):

            @pl.when(k == steps - CHUNKS // nx + i * CHUNKS // nx // PIECES)
            def _(i=i):
                other = w_ref.at[1, pl.ds(((1 - x) * PIECES + i) * piece, piece)]
                pltpu.make_async_copy(other, other, wx.at[i]).wait()

        which = k // CHUNKS
        part_of = lax.rem(k + which * x * (CHUNKS // nx), CHUNKS)

        def channel(c, peak):
            w = w_ref[which, part_of * per + c].reshape(antennas2, beams).T
            power = None
            for h in range(nx):
                v = vrecv[k, h * group : (h + 1) * group, c].reshape(antennas2, half)
                mixed = jnp.dot(mix_ref[...], v, preferred_element_type=jnp.float32)
                mixed = mixed.astype(jnp.bfloat16)
                re = jnp.dot(w, mixed[:antennas2], preferred_element_type=jnp.float32)
                im = jnp.dot(w, mixed[antennas2:], preferred_element_type=jnp.float32)
                part = re * re + im * im
                power = part if power is None else power + part
            own = beams // ng
            packs = own // 8
            power = power.reshape(ng, packs, 8, half)
            total = None
            for m in range(packs):
                p = power[:, m].reshape(ng * 8, half)
                high = p.astype(jnp.bfloat16)
                low = (p - high.astype(jnp.float32)).astype(jnp.bfloat16)
                t = jnp.dot(high, gather_ref[m], preferred_element_type=jnp.float32)
                t += jnp.dot(low, gather_ref[m], preferred_element_type=jnp.float32)
                total = t if total is None else total + t
            total = total.reshape(ng, 8, 128)
            work[:, pl.ds(c, 1)] = total[:, None]
            return jnp.maximum(peak, jnp.max(total, axis=0))

        peak = lax.fori_loop(0, per, channel, jnp.zeros((8, 128), jnp.float32))
        peak = jnp.maximum(jnp.max(peak, keepdims=True), FLOOR)
        code = work[...].reshape(ng, per * 8, 128) * (TOP / peak)[None]
        code = code * code
        code = code * code
        code = code * code
        near = code.astype(jnp.bfloat16).astype(jnp.float32)
        pbuf[k] = jnp.where(code < near, -near, near).astype(jnp.bfloat16)
        row = lax.broadcasted_iota(jnp.int32, peaks.shape, 0)
        lane = lax.broadcasted_iota(jnp.int32, peaks.shape, 1)
        own_row = lax.rem(side + which, 2)
        first = u * chans + part_of * per
        held = (row == own_row) & (lane >= first) & (lane < first + per)
        peaks[...] = jnp.where(held, peak, peaks[...])

        @pl.when(k == 0)
        def _():
            pl.semaphore_wait(cross, 1)

        def send(i, _):
            send_powers(k, (1 - side) * group + i)
            return 0

        @pl.when(side == 0)
        def _():
            send_near(k)

        lax.fori_loop(0, group, send, 0)

        @pl.when(~last & (side == 1))
        def _():
            send_near(k)

        @pl.when(last & (k >= NEAR))
        def _():
            send_near(k - NEAR)

        return 0

    peaks[...] = jnp.zeros_like(peaks)
    lax.fori_loop(0, steps, step, 0)

    pltpu.make_async_copy(peaks, peak_ref.at[side, u], mget).start()

    def send_peaks(i, _):
        pltpu.make_async_remote_copy(
            src_ref=peaks,
            dst_ref=peak_ref.at[side, u],
            send_sem=msend,
            recv_sem=mget,
            device_id=(x, lax.rem(g + i, ng)),
            device_id_type=MESH,
        ).start()
        return 0

    lax.fori_loop(1, ng, send_peaks, 0)

    @pl.when(last)
    def _():
        def late(k, _):
            send_near(k)
            return 0

        lax.fori_loop(steps - NEAR, steps, late, 0)

    def decode(k, _):
        pltpu.make_async_copy(pbuf.at[k], pbuf.at[k], pget.at[k]).wait()
        which = k // CHUNKS
        part_of = lax.rem(k + which * x * (CHUNKS // nx), CHUNKS)
        for other in range(2):
            span = pl.ds((other + which) % 2 * group, group)
            code = codes[other, span, part_of].astype(jnp.float32)
            near = jnp.abs(code)
            gap = (near * NEXT).astype(jnp.bfloat16).astype(jnp.float32) - near
            near = near + jnp.where(code < 0, -0.25, 0.25) * gap
            plain[other, span, part_of] = jnp.exp(jnp.log(near) * 0.125)
            pltpu.make_async_copy(
                plain.at[other, span, part_of],
                out_ref.at[other, span, part_of],
                out_sem,
            ).start()
        return 0

    lax.fori_loop(0, steps, decode, 0)
    pltpu.make_async_copy(peak_ref, peak_ref, mget).wait()
    pltpu.make_async_copy(out_ref, out_ref, out_sem).wait()
    for k in range(steps):
        sent = sbuf.at[k, pl.ds(0, dests - 1)]
        pltpu.make_async_copy(sent, sent, vsend.at[k]).wait()
    sent = pbuf.at[:, pl.ds(0, ng - 1)]
    pltpu.make_async_copy(sent, sent, psend).wait()
    sent = peak_ref.at[:, pl.ds(0, group - 1)]
    pltpu.make_async_copy(sent, sent, msend).wait()
    sent = peak_ref.at[0, pl.ds(0, 1)]
    pltpu.make_async_copy(sent, sent, msend).wait()
    sent = w_ref.at[1, pl.ds(0, PIECES * piece)]
    pltpu.make_async_copy(sent, sent, wsend).wait()
    pltpu.make_async_copy(sent, sent, relay_sem).wait()


def spread_kernel(in_ref, peak_ref, out_ref, block, sem):
    channels, bins = out_ref.shape[3], out_ref.shape[2]
    packs = 128 // bins

    def copies(q, r):
        for m in range(packs):
            yield pltpu.make_async_copy(block.at[q, m * 8 + r], out_ref.at[q, m * 8 + r], sem)

    before = None
    for q in range(2):
        scale = jnp.sum(peak_ref[q], axis=0) * (1.0 / TOP)
        scale = jnp.concatenate([scale[0:1], scale[1:2]], axis=1)
        for r in range(8):
            lanes = in_ref[q, pl.ds(r, channels, stride=8), :].T * scale
            for m in range(packs):
                block[q, m * 8 + r] = lanes[m * bins : (m + 1) * bins]
            if before is not None:
                for copy in copies(*before):
                    copy.start()
            before = (q, r)
    for copy in copies(*before):
        copy.start()
    pltpu.make_async_copy(block, out_ref, sem).wait()


def on_device(nx, ng, voltages, weights):
    v = voltages[0]
    streams, parts, channels, samples = v.shape
    rows, chans, half = streams * parts, channels // ng, samples // nx
    per = chans // CHUNKS
    group = ng // 2
    antennas = group * streams
    beams = weights.shape[3]
    own = beams // ng
    packs = own // 8
    bins = half // 8

    turned_weights = jnp.swapaxes(weights, 3, 4)
    hbm = pl.BlockSpec(memory_space=pltpu.HBM)
    anywhere = pl.BlockSpec(memory_space=pl.ANY)
    packed, peaks = pl.pallas_call(
        functools.partial(kernel, nx, ng),
        out_shape=(
            jax.ShapeDtypeStruct((2, ng, CHUNKS, per * 8, 128), jnp.float32),
            jax.ShapeDtypeStruct((2, group, 2, 128), jnp.float32),
        ),
        in_specs=[hbm, hbm],
        out_specs=(anywhere, anywhere),
        scratch_shapes=[
            pltpu.VMEM((rows * chans, rows * chans), jnp.bfloat16),
            pltpu.VMEM((4 * antennas, 2 * antennas), jnp.bfloat16),
            pltpu.VMEM((packs, half, 128), jnp.bfloat16),
            pltpu.VMEM((2 * group, streams, parts, chans, samples), jnp.bfloat16),
            pltpu.VMEM((2 * CHUNKS, nx * group, per, rows, half), jnp.bfloat16),
            pltpu.VMEM((2 * CHUNKS, nx * group, per, rows, half), jnp.bfloat16),
            pltpu.VMEM(turned_weights.shape, jnp.bfloat16),
            pltpu.VMEM((ng, per, 8, 128), jnp.float32),
            pltpu.VMEM((2 * CHUNKS, ng, per * 8, 128), jnp.bfloat16),
            pltpu.VMEM((2, ng, CHUNKS, per * 8, 128), jnp.bfloat16),
            pltpu.VMEM((2, ng, CHUNKS, per * 8, 128), jnp.float32),
            pltpu.VMEM((2, 128), jnp.float32),
            pltpu.SemaphoreType.DMA((2 * group,)),
            pltpu.SemaphoreType.REGULAR,
            pltpu.SemaphoreType.DMA,
            pltpu.SemaphoreType.DMA,
            pltpu.SemaphoreType.DMA((PIECES,)),
            pltpu.SemaphoreType.DMA,
            pltpu.SemaphoreType.DMA((PIECES,)),
            pltpu.SemaphoreType.DMA((2 * CHUNKS,)),
            pltpu.SemaphoreType.DMA((2 * CHUNKS,)),
            pltpu.SemaphoreType.DMA,
            pltpu.SemaphoreType.DMA((2 * CHUNKS,)),
            pltpu.SemaphoreType.DMA,
            pltpu.SemaphoreType.DMA,
            pltpu.SemaphoreType.DMA,
        ],
        compiler_params=pltpu.CompilerParams(
            collective_id=0, has_side_effects=True, vmem_limit_bytes=VMEM
        ),
    )(v, turned_weights)

    spread = pl.pallas_call(
        spread_kernel,
        out_shape=jax.ShapeDtypeStruct((2, own, bins, channels), jnp.float32),
        in_specs=[pl.BlockSpec(memory_space=pltpu.VMEM)] * 2,
        out_specs=anywhere,
        scratch_shapes=[
            pltpu.VMEM((2, own, bins, channels), jnp.float32),
            pltpu.SemaphoreType.DMA,
        ],
        compiler_params=pltpu.CompilerParams(vmem_limit_bytes=VMEM),
    )(packed.reshape(2, channels * 8, 128), peaks)
    return spread.transpose(3, 0, 1, 2)


def solution(mesh):
    nx, ng = mesh.shape["ta"], mesh.shape["gx"]

    def body(voltages, weights):
        _, streams, parts, channels, samples = voltages.shape
        rows, chans, half = streams * parts, channels // ng, samples // nx
        own = weights.shape[3] // ng
        fits = (
            nx == 2
            and rows % 16 == 0
            and chans % 16 == 0
            and half % 128 == 0
            and own % 8 == 0
            and (own // 8) * (half // 8) == 128
            and ng % 2 == 0
            and ng & (ng - 1) == 0
            and ng * chans == 256
        )
        if fits:
            return on_device(nx, ng, voltages, weights)
        return plain_on_device(voltages, weights)

    in_specs = (P("ta", "gx", None, None, None), P(None, "gx", None, None, None))
    out_specs = P(None, None, "gx", "ta")
    return jax.shard_map(
        body, mesh=mesh, in_specs=in_specs, out_specs=out_specs, check_vma=False
    )
```
